64 devices in a mesh: dp: 4 (over x, y), tp: 16 (over z, core).
Axes of the slice: x: 2, y: 2, z: 8, core: 2. Of those that a mesh axis runs over, the one named last changes fastest.
The devices are a block of a 4x4x8 slice.
Arguments:
- hidden: bfloat16 [4096, 2048], P('dp'), parts along dimension 0
- tokens: int32 [4096], P('dp'), parts along dimension 0
- embedding: bfloat16 [49152, 2048], P('tp')
- head_w: bfloat16 [2048, 49152], P(None, 'tp')
- h_norm: float32 [2048], replicated
- e_norm: float32 [2048], replicated
- f_norm: float32 [2048], replicated
- o_norm: float32 [2048], replicated
- proj_w: bfloat16 [4096, 2048], P(None, 'tp')
- w_gate: bfloat16 [2048, 8192], P(None, 'tp')
- w_up: bfloat16 [2048, 8192], P(None, 'tp')
- w_down: bfloat16 [8192, 2048], P('tp')
Outputs:
- output 1: bfloat16 [4096, 2048], P('dp'), parts along dimension 0
- output 2: float32 [4096, 49152], P('dp', 'tp'), parts along dimension 0
There are 4 independent parts. The reference program is written for one: setup_inputs(seed, part) draws one part's arguments, and reference() takes and returns one part's arrays. A program takes and returns all parts, laid end to end along the dimension named above; an argument that names none is the same for every part.
All inputs are finite; a program needn't handle non-finite values.
Results may differ from the reference program's by a relative error of at most 0.0111877.
Values are sent between devices in bfloat16 or wider.
A program may use at most 768 MiB of HBM per device.

```python
import jax
import jax.numpy as jnp
from jax import lax

MODEL_DIM = 2048
VOCAB_SIZE = 49152
FFN_DIM = 8192
BATCH_ROWS = 1024

HOT_WIDTH = VOCAB_SIZE // 32
NORM_EPS = 1e-6


def draw_tokens(key_in):
    sub_keys = jax.random.split(key_in, 4)
    hot_starts = jax.random.randint(sub_keys[0], (2,), 0, VOCAB_SIZE - HOT_WIDTH + 1)
    choice = jax.random.randint(sub_keys[1], (BATCH_ROWS,), 0, 4)
    offsets = jax.random.randint(sub_keys[2], (BATCH_ROWS,), 0, HOT_WIDTH)
    spread = jax.random.randint(sub_keys[3], (BATCH_ROWS,), 0, VOCAB_SIZE)
    hot_ids = jnp.where(choice == 3, hot_starts[1], hot_starts[0]) + offsets
    token_ids = jnp.where(choice == 0, spread, hot_ids)
    return token_ids.at[0].set(0).at[BATCH_ROWS - 1].set(VOCAB_SIZE - 1).astype(jnp.int32)


def setup_inputs(seed: int = 0, part: int = 0) -> dict:
    root_key = jax.random.key(seed)
    part_keys = jax.random.split(jax.random.fold_in(root_key, part), 2)
    weight_keys = jax.random.split(root_key, 10)
    hidden = (2.0 * jax.random.normal(part_keys[0], (BATCH_ROWS, MODEL_DIM), jnp.float32)).astype(jnp.bfloat16)
    tokens = draw_tokens(part_keys[1])
    embedding = jax.random.normal(weight_keys[0], (VOCAB_SIZE, MODEL_DIM), jnp.float32).astype(jnp.bfloat16)
    head_w = (jax.random.normal(weight_keys[1], (MODEL_DIM, VOCAB_SIZE), jnp.float32) * (1.5 * MODEL_DIM ** -0.5)).astype(jnp.bfloat16)
    h_norm = 1.0 + 0.5 * jax.random.normal(weight_keys[2], (MODEL_DIM,), jnp.float32)
    e_norm = 1.0 + 0.5 * jax.random.normal(weight_keys[3], (MODEL_DIM,), jnp.float32)
    f_norm = 1.0 + 0.5 * jax.random.normal(weight_keys[4], (MODEL_DIM,), jnp.float32)
    o_norm = 1.0 + 0.5 * jax.random.normal(weight_keys[5], (MODEL_DIM,), jnp.float32)
    proj_w = (jax.random.normal(weight_keys[6], (2 * MODEL_DIM, MODEL_DIM), jnp.float32) * (2 * MODEL_DIM) ** -0.5).astype(jnp.bfloat16)
    w_gate = (jax.random.normal(weight_keys[7], (MODEL_DIM, FFN_DIM), jnp.float32) * MODEL_DIM ** -0.5).astype(jnp.bfloat16)
    w_up = (jax.random.normal(weight_keys[8], (MODEL_DIM, FFN_DIM), jnp.float32) * MODEL_DIM ** -0.5).astype(jnp.bfloat16)
    w_down = (jax.random.normal(weight_keys[9], (FFN_DIM, MODEL_DIM), jnp.float32) * FFN_DIM ** -0.5).astype(jnp.bfloat16)
    return {"hidden": hidden, "tokens": tokens, "embedding": embedding, "head_w": head_w, "h_norm": h_norm, "e_norm": e_norm, "f_norm": f_norm, "o_norm": o_norm, "proj_w": proj_w, "w_gate": w_gate, "w_up": w_up, "w_down": w_down}


def rms_norm(values, norm_gain):
    wide_vals = values.astype(jnp.float32)
    inv_rms = lax.rsqrt(jnp.mean(wide_vals * wide_vals, axis=-1, keepdims=True) + NORM_EPS)
    return wide_vals * inv_rms * norm_gain


def reference(hidden, tokens, embedding, head_w, h_norm, e_norm, f_norm, o_norm, proj_w, w_gate, w_up, w_down):
    emb_rows = jnp.take(embedding, tokens, axis=0)
    joined = jnp.concatenate([rms_norm(hidden, h_norm), rms_norm(emb_rows, e_norm)], axis=-1).astype(jnp.bfloat16)
    proj_full = jnp.dot(joined, proj_w, preferred_element_type=jnp.float32).astype(jnp.bfloat16)
    normed = rms_norm(proj_full, f_norm).astype(jnp.bfloat16)
    gate_val = jnp.dot(normed, w_gate, preferred_element_type=jnp.float32)
    up_val = jnp.dot(normed, w_up, preferred_element_type=jnp.float32)
    act_val = (jax.nn.silu(gate_val) * up_val).astype(jnp.bfloat16)
    down_val = jnp.dot(act_val, w_down, preferred_element_type=jnp.float32)
    new_u = (proj_full.astype(jnp.float32) + down_val).astype(jnp.bfloat16)
    out_norm = rms_norm(new_u, o_norm).astype(jnp.bfloat16)
    logits = jnp.dot(out_norm, head_w, preferred_element_type=jnp.float32)
    log_total = jax.nn.logsumexp(logits, axis=-1, keepdims=True)
    return new_u, logits - log_total
```

```python
import functools

import jax
import jax.numpy as jnp
from jax import lax
from jax.experimental import pallas as pl
from jax.experimental.pallas import tpu as pltpu
from jax.sharding import PartitionSpec as P

NORM_EPS = 1e-6
BF16 = jnp.bfloat16
F32 = jnp.float32
GROUP_ROWS = 256
CORES = 2
SEND_R, SEND_L, FROM_L, FROM_R = range(4)
E_RS, E_AG, P_AG, D_RS, U_AG = range(5)


def norm_rows(values, gain):
    wide = values.astype(F32)
    inv = lax.rsqrt(jnp.mean(wide * wide, axis=-1, keepdims=True) + NORM_EPS)
    return wide * inv * gain


def aligned(index, size):
    return pl.ds(pl.multiple_of(index * size, size), size)


def tile_of(width, most):
    return min(width, most)


def step_kernel(
    n_tp, tok, hg, eg, fg, og, hid_h, emb_h, head_h, pw_h, wg_h, wu_h, wd_h,
    u_h, z_h, lse,
    big, hid, pu, land, ebuf, pbuf, part, pw, wg, wu, wd, erl, err, drl, drr,
    onehot, nbuf, abuf, obuf, zst, mst, sst, stats,
    ring, xsend, xrecv, wsend, wrecv, ssend, srecv, lsem, bsem, hsem, zsem, usem,
):
    groups, half_rows, dim = hid.shape
    chips = n_tp // CORES
    hops = chips // 2
    rows = CORES * half_rows
    blk = half_rows // chips
    hcol = dim // 2
    hrow = half_rows // 2
    pcols = pw.shape[1] // CORES
    fcols = wg.shape[1] // CORES
    vocab = zst.shape[1]
    q = big.shape[1]
    n_vq, n_dq = vocab // q, dim // q

    me = lax.axis_index("tp")
    z, k = me // CORES, lax.rem(me, CORES)
    other = 1 - k
    sib = z * CORES + other
    right = lax.rem(me + CORES, n_tp)
    left = lax.rem(me + n_tp - CORES, n_tp)

    def chip(offset):
        return lax.rem(z + offset + chips, chips)

    def remote(src, dst, ssem, rsem, dev):
        return pltpu.make_async_remote_copy(
            src_ref=src, dst_ref=dst, send_sem=ssem, recv_sem=rsem,
            device_id={"tp": dev}, device_id_type=pl.DeviceIdType.MESH,
        )

    def emb_copy(i, j):
        return pltpu.make_async_copy(
            emb_h.at[pl.ds(i * q, q), pl.ds(j * q, q)], big.at[i * n_dq + j], bsem.at[i * n_dq + j])

    def head_copy(i, j):
        return pltpu.make_async_copy(
            head_h.at[pl.ds(i * q, q), pl.ds(j * q, q)], big.at[i * n_vq + j], hsem.at[i * n_vq + j])

    def hid_copy(g):
        return pltpu.make_async_copy(
            hid_h.at[pl.ds(pl.multiple_of(g * rows + k * half_rows, half_rows), half_rows)], hid.at[g], lsem.at[4 + g])

    own_pw = pw.at[:, aligned(k, pcols)]
    own_wg = wg.at[:, aligned(k, fcols)]
    own_wu = wu.at[:, aligned(k, fcols)]
    own_wd = wd.at[aligned(k, fcols), :]
    oth_pw = pw.at[:, aligned(other, pcols)]
    oth_wg = wg.at[:, aligned(other, fcols)]
    oth_wu = wu.at[:, aligned(other, fcols)]
    oth_wd = wd.at[aligned(other, fcols), :]
    w_local = [pltpu.make_async_copy(s, d, lsem.at[i]) for i, (s, d) in enumerate(
        [(pw_h, own_pw), (wg_h, own_wg), (wu_h, own_wu), (wd_h, own_wd)])]
    w_send = [remote(r, r, wsend.at[i], wrecv.at[i], sib) for i, r in enumerate([own_pw, own_wg, own_wu, own_wd])]
    w_recv = [remote(r, r, wsend.at[i], wrecv.at[i], sib) for i, r in enumerate([oth_pw, oth_wg, oth_wu, oth_wd])]

    for i in range(n_vq):
        for j in range(n_dq):
            emb_copy(i, j).start()
    for c in w_local:
        c.start()

    @pl.loop(0, groups)
    def _(g):
        hid_copy(g).start()

    barrier = pltpu.get_barrier_semaphore()
    for d in range(1, n_tp):
        pl.semaphore_signal(barrier, inc=1, device_id={"tp": lax.rem(me + d, n_tp)}, device_id_type=pl.DeviceIdType.MESH)
    pl.semaphore_wait(barrier, n_tp - 1)

    def e_blk(g, o, h):
        cols = pl.ds(0, dim) if h is None else pl.ds(h * hcol, hcol)
        return ebuf.at[g, aligned(o, blk), cols]

    def p_blk(g, o, h):
        r = pl.ds(0, half_rows) if h is None else pl.ds(h * hrow, hrow)
        return pbuf.at[g, r, aligned(o, CORES * pcols)]

    def u_blk(g, o, h):
        cols = pl.ds(0, dim) if h is None else pl.ds(h * hcol, hcol)
        return pu.at[g, pl.ds(pl.multiple_of(k * half_rows + o * blk, blk), blk), cols]

    def ag_pair(c, block, g, s):
        last = s == hops
        r = block(g, chip(-(s - 1)), 0 if last else None)
        l = block(g, chip(s - 1), 1 if last else None)
        return (remote(r, r, ring.at[c, SEND_R, g, s - 1], ring.at[c, FROM_L, g, s - 1], right),
                remote(l, l, ring.at[c, SEND_L, g, s - 1], ring.at[c, FROM_R, g, s - 1], left))

    def ag_wait(c, block, g, s):
        last = s == hops
        r = block(g, chip(-s), 0 if last else None)
        l = block(g, chip(s), 1 if last else None)
        return (remote(r, r, ring.at[c, SEND_R, g, s - 1], ring.at[c, FROM_L, g, s - 1], right),
                remote(l, l, ring.at[c, SEND_L, g, s - 1], ring.at[c, FROM_R, g, s - 1], left))

    def ag_send(c, block, g, s):
        for cp in ag_pair(c, block, g, s):
            cp.start()

    def ag_step(c, block, g, s):
        got, send = ag_wait(c, block, g, s - 1), ag_pair(c, block, g, s)
        for a, b in zip(got, send):
            a.wait_recv()
            b.start()

    def rs_part(ref, h):
        return ref if h is None else ref.at[:, pl.ds(h * hcol, hcol)]

    def rs_pair(c, own, lands, g, s):
        out = []
        for kind, frm, side, dev, h1, sign in ((SEND_R, FROM_L, 0, right, 0, 1), (SEND_L, FROM_R, 1, left, 1, -1)):
            h = h1 if s == 1 else None
            dst = rs_part(lands[side].at[g, s - 1], h)
            src = rs_part(own.at[g, aligned(chip(sign * hops), blk)], h) if s == 1 else lands[side].at[g, s - 2]
            out.append(remote(src, dst, ring.at[c, kind, g, s - 1], ring.at[c, frm, g, s - 1], dev))
        return out

    def rs_wait(c, own, lands, g, s):
        return rs_pair(c, own, lands, g, s)

    def rs_first(c, own, lands, g):
        for cp in rs_pair(c, own, lands, g, 1):
            cp.start()

    def rs_step(c, own, lands, g, s):
        got, send = rs_wait(c, own, lands, g, s - 1), rs_pair(c, own, lands, g, s)
        for side, sign in ((0, 1), (1, -1)):
            got[side].wait_recv()
            o = aligned(chip(sign * (hops + 1 - s)), blk)
            slot = lands[side].at[g, s - 2]
            if s == 2:
                for h in range(2):
                    c_ = slice(h * hcol, (h + 1) * hcol)
                    mine = own[g, o, c_]
                    slot[:, c_] = slot[:, c_] + mine if h == side else mine
            else:
                slot[...] = slot[...] + own[g, o, :]
            send[side].start()

    def rs_sum(c, own, lands, g):
        for cp in rs_wait(c, own, lands, g, hops):
            cp.wait_recv()
        mine = own[g, aligned(z, blk), :]
        return lands[0][g, hops - 1].astype(F32) + mine.astype(F32) + lands[1][g, hops - 1].astype(F32)

    e_lands, d_lands = (erl, err), (drl, drr)

    def pick_swap(g):
        return remote(pu.at[g, aligned(other, half_rows)], land.at[g], xsend.at[0, g], xrecv.at[0, g], sib)

    def u_swap(g, c):
        r = pu.at[g, aligned(c, half_rows)]
        return remote(r, r, xsend.at[1, g], xrecv.at[1, g], sib)

    def stat_send(g, d):
        return remote(stats.at[g, me], stats.at[g, me], ssend.at[g, d], srecv.at[g, d], lax.rem(me + d, n_tp))

    def stat_wait(g, d):
        src = lax.rem(me + n_tp - d, n_tp)
        return remote(stats.at[g, src], stats.at[g, src], ssend.at[g, d], srecv.at[g, d], lax.rem(me + d, n_tp))

    def z_copy(g, j):
        return pltpu.make_async_copy(
            zst.at[:, pl.ds(j * q, q)], z_h.at[aligned(g, rows), pl.ds(j * q, q)], zsem.at[j])

    def u_copy(g):
        return pltpu.make_async_copy(pu.at[g], u_h.at[aligned(g, rows)], usem.at[g])

    def picks(g):
        @pl.when(g == 0)
        def _():
            for i in range(n_vq):
                for j in range(n_dq):
                    emb_copy(i, j).wait()

        ids = tok[aligned(g, rows), :] - me * vocab
        lanes = ids.shape[1]
        lane = lax.broadcasted_iota(jnp.int32, ids.shape, 1)

        @pl.loop(0, vocab // lanes)
        def _(j):
            onehot[:, aligned(j, lanes)] = jnp.where(ids - j * lanes == lane, 1.0, 0.0).astype(BF16)

        tn = tile_of(q, 512)
        for j in range(n_dq):
            @pl.loop(0, q // tn)
            def _(t):
                acc = None
                for i in range(n_vq):
                    d = jnp.dot(onehot[:, i * q:(i + 1) * q], big[i * n_dq + j, :, aligned(t, tn)], preferred_element_type=F32)
                    acc = d if acc is None else acc + d
                pu[g, :, pl.ds(pl.multiple_of(j * q + t * tn, tn), tn)] = acc.astype(BF16)

        pick_swap(g).start()

        @pl.when(g == groups - 1)
        def _():
            for i in range(n_dq):
                for j in range(n_vq):
                    head_copy(i, j).start()

        @pl.when(g == 0)
        def _():
            w_local[0].wait()
            w_send[0].start()

    def pick_sum(g):
        pick_swap(g).wait_recv()

        @pl.loop(0, chips)
        def _(i):
            r = aligned(i, blk)
            land[g, r, :] = land[g, r, :] + pu[g, pl.ds(pl.multiple_of(k * half_rows + i * blk, blk), blk), :]

        rs_first(E_RS, land, e_lands, g)

    def e_norm(g):
        pick_swap(g).wait_send()
        ebuf[g, aligned(z, blk), :] = norm_rows(rs_sum(E_RS, land, e_lands, g), eg[...]).astype(BF16)
        ag_send(E_AG, e_blk, g, 1)

    def h_norm(g):
        hid_copy(g).wait()

        @pl.loop(0, chips)
        def _(i):
            r = aligned(i, blk)
            hid[g, r, :] = norm_rows(hid[g, r, :], hg[...]).astype(BF16)

        @pl.when(g == 0)
        def _():
            for i in range(1, 4):
                w_local[i].wait()
                w_send[i].start()

    def project(g):
        for cp in ag_wait(E_AG, e_blk, g, hops):
            cp.wait_recv()

        @pl.when(g == 0)
        def _():
            w_recv[0].wait_recv()

        out = jnp.dot(hid[g], pw[:dim, :], preferred_element_type=F32)
        out += jnp.dot(ebuf[g], pw[dim:, :], preferred_element_type=F32)
        pbuf[g, :, aligned(z, CORES * pcols)] = out.astype(BF16)
        ag_send(P_AG, p_blk, g, 1)

    def feed_forward(g):
        for cp in ag_wait(P_AG, p_blk, g, hops):
            cp.wait_recv()

        @pl.when(g == 0)
        def _():
            for i in range(1, 4):
                w_recv[i].wait_recv()

        @pl.loop(0, chips)
        def _(i):
            r = aligned(i, blk)
            nbuf[r, :] = norm_rows(pbuf[g, r, :], fg[...]).astype(BF16)

        width = wg.shape[1]
        tn = tile_of(width, 256)

        @pl.loop(0, width // tn)
        def _(t):
            c = aligned(t, tn)
            gate = jnp.dot(nbuf[...], wg[:, c], preferred_element_type=F32)
            up = jnp.dot(nbuf[...], wu[:, c], preferred_element_type=F32)
            abuf[:, c] = (jax.nn.silu(gate) * up).astype(BF16)

        tm = tile_of(dim, 512)

        @pl.loop(0, dim // tm)
        def _(t):
            c = aligned(t, tm)
            part[g, :, c] = jnp.dot(abuf[...], wd[:, c], preferred_element_type=F32)

        rs_first(D_RS, part, d_lands, g)

    def new_u(g):
        total = rs_sum(D_RS, part, d_lands, g)
        total = pbuf[g, aligned(z, blk), :].astype(F32) + total
        pu[g, pl.ds(pl.multiple_of(k * half_rows + z * blk, blk), blk), :] = total.astype(BF16)
        ag_send(U_AG, u_blk, g, 1)

    def u_done(g):
        for cp in ag_wait(U_AG, u_blk, g, hops):
            cp.wait_recv()
        u_swap(g, k).start()

    def head(g):
        u_swap(g, other).wait_recv()
        u_copy(g).start()

        @pl.when(g == 0)
        def _():
            for i in range(n_dq):
                for j in range(n_vq):
                    head_copy(i, j).wait()

        @pl.loop(0, rows // blk)
        def _(i):
            r = aligned(i, blk)
            obuf[r, :] = norm_rows(pu[g, r, :], og[...]).astype(BF16)

        tn = tile_of(q, 512)
        for j in range(n_vq):
            @pl.when(g > 0)
            def _():
                z_copy(g - 1, j).wait()

            @pl.loop(0, q // tn)
            def _(t):
                acc = None
                for i in range(n_dq):
                    d = jnp.dot(obuf[:, i * q:(i + 1) * q], big[i * n_vq + j, :, aligned(t, tn)], preferred_element_type=F32)
                    acc = d if acc is None else acc + d
                zst[:, pl.ds(pl.multiple_of(j * q + t * tn, tn), tn)] = acc

            z_copy(g, j).start()

        @pl.loop(0, rows // blk)
        def _(i):
            r = aligned(i, blk)
            zz = zst[r, :]
            m = jnp.max(zz, axis=-1, keepdims=True)
            s = jnp.sum(jnp.exp(zz - m), axis=-1, keepdims=True)
            mst[r, :] = jnp.broadcast_to(m, (blk, mst.shape[1]))
            sst[r, :] = jnp.broadcast_to(s, (blk, sst.shape[1]))

        mt, st = mst[...].T, sst[...].T
        lanes = stats.shape[3]
        n = rows // lanes
        for i in range(n):
            c = slice(i * lanes, (i + 1) * lanes)
            stats[g, me, i:i + 1, :] = mt[0:1, c]
            stats[g, me, n + i:n + i + 1, :] = st[0:1, c]
        for d in range(1, n_tp):
            stat_send(g, d).start()

    def total_lse(g):
        for d in range(1, n_tp):
            stat_wait(g, d).wait_recv()
        n = rows // stats.shape[3]
        ms = [stats[g, i, 0:n, :] for i in range(n_tp)]
        top = functools.reduce(jnp.maximum, ms)
        tot = functools.reduce(jnp.add, [stats[g, i, n:2 * n, :] * jnp.exp(ms[i] - top) for i in range(n_tp)])
        lse[g, 0:n, :] = top + jnp.log(tot)

    stages = [picks, pick_sum]
    stages += [functools.partial(rs_step, E_RS, land, e_lands, s=s) for s in range(2, hops + 1)]
    stages += [e_norm]
    stages += [functools.partial(ag_step, E_AG, e_blk, s=s) for s in range(2, hops + 1)]
    h_at = len(stages) - 1
    stages += [project]
    stages += [functools.partial(ag_step, P_AG, p_blk, s=s) for s in range(2, hops + 1)]
    stages += [feed_forward]
    stages += [functools.partial(rs_step, D_RS, part, d_lands, s=s) for s in range(2, hops + 1)]
    stages += [new_u]
    stages += [functools.partial(ag_step, U_AG, u_blk, s=s) for s in range(2, hops + 1)]
    stages += [u_done]
    head_at = len(stages)
    stages += [head, total_lse]
    order = [i for i in range(len(stages) - 1, -1, -1) if i not in (head_at,)] + [head_at]

    @pl.loop(0, groups + len(stages) - 1)
    def _(t):
        for i in order:
            g = t - i

            @pl.when((g >= 0) & (g < groups))
            def _():
                stages[i](g=g)
                if i == h_at:
                    h_norm(g)

    for cp in w_send:
        cp.wait_send()
    for j in range(n_vq):
        z_copy(groups - 1, j).wait()

    @pl.loop(0, groups)
    def _(g):
        for s in range(1, hops + 1):
            for cp in rs_pair(E_RS, land, e_lands, g, s) + rs_pair(D_RS, part, d_lands, g, s):
                cp.wait_send()
            for c, b in ((E_AG, e_blk), (P_AG, p_blk), (U_AG, u_blk)):
                for cp in ag_pair(c, b, g, s):
                    cp.wait_send()
        u_swap(g, k).wait_send()
        for d in range(1, n_tp):
            stat_send(g, d).wait_send()
        u_copy(g).wait()


def draft_call(n_tp, hidden, tokens, embedding, head_w, h_norm, e_norm, f_norm, o_norm, proj_w, w_gate, w_up, w_down):
    batch, dim = hidden.shape
    vocab = embedding.shape[0]
    pcols, fcols = proj_w.shape[1], w_gate.shape[1]
    groups = batch // GROUP_ROWS
    half_rows = GROUP_ROWS // CORES
    chips = n_tp // CORES
    hops = chips // 2
    blk = half_rows // chips
    q = dim // 2
    lanes = 128
    tok = jnp.broadcast_to(tokens[:, None], (batch, lanes))
    vm = pl.BlockSpec(memory_space=pltpu.VMEM)
    anyspec = pl.BlockSpec(memory_space=pl.ANY)
    dma = pltpu.SemaphoreType.DMA
    n_big = (vocab // q) * (dim // q)
    flops = 2 * batch * (2 * dim * vocab + 2 * dim * pcols + 3 * dim * fcols)
    return pl.pallas_call(
        functools.partial(step_kernel, n_tp),
        out_shape=(
            jax.ShapeDtypeStruct((batch, dim), BF16),
            jax.ShapeDtypeStruct((batch, vocab), F32),
            jax.ShapeDtypeStruct((groups, 8, lanes), F32),
        ),
        in_specs=[vm] * 5 + [anyspec] * 7,
        out_specs=(anyspec, anyspec, vm),
        scratch_shapes=[
            pltpu.VMEM((n_big, q, q), BF16),
            pltpu.VMEM((groups, half_rows, dim), BF16),
            pltpu.VMEM((groups, GROUP_ROWS, dim), BF16),
            pltpu.VMEM((groups, half_rows, dim), BF16),
            pltpu.VMEM((groups, half_rows, dim), BF16),
            pltpu.VMEM((groups, half_rows, dim), BF16),
            pltpu.VMEM((groups, half_rows, dim), F32),
            pltpu.VMEM((2 * dim, CORES * pcols), BF16),
            pltpu.VMEM((dim, CORES * fcols), BF16),
            pltpu.VMEM((dim, CORES * fcols), BF16),
            pltpu.VMEM((CORES * fcols, dim), BF16),
            pltpu.VMEM((groups, hops, blk, dim), BF16),
            pltpu.VMEM((groups, hops, blk, dim), BF16),
            pltpu.VMEM((groups, hops, blk, dim), F32),
            pltpu.VMEM((groups, hops, blk, dim), F32),
            pltpu.VMEM((GROUP_ROWS, vocab), BF16),
            pltpu.VMEM((half_rows, dim), BF16),
            pltpu.VMEM((half_rows, CORES * fcols), BF16),
            pltpu.VMEM((GROUP_ROWS, dim), BF16),
            pltpu.VMEM((GROUP_ROWS, vocab), F32),
            pltpu.VMEM((GROUP_ROWS, lanes), F32),
            pltpu.VMEM((GROUP_ROWS, lanes), F32),
            pltpu.VMEM((groups, n_tp, 8, lanes), F32),
            dma((5, 4, groups, hops)),
            dma((2, groups)),
            dma((2, groups)),
            dma((4,)),
            dma((4,)),
            dma((groups, n_tp)),
            dma((groups, n_tp)),
            dma((4 + groups,)),
            dma((n_big,)),
            dma((n_big,)),
            dma((vocab // q,)),
            dma((groups,)),
        ],
        compiler_params=pltpu.CompilerParams(
            collective_id=0, has_side_effects=True, vmem_limit_bytes=67043328),
        cost_estimate=pl.CostEstimate(flops=flops, bytes_accessed=70 << 20, transcendentals=0),
        name="draft_step",
    )(tok, h_norm[None], e_norm[None], f_norm[None], o_norm[None], hidden, embedding, head_w, proj_w, w_gate, w_up, w_down)


def solution(mesh):
    n_tp = mesh.shape["tp"]

    def draft_step(hidden, *rest):
        new_u, logits, lse = draft_call(n_tp, hidden, *rest)
        groups = lse.shape[0]
        lse_rows = lse[:, : GROUP_ROWS // lse.shape[2], :].reshape(hidden.shape[0])
        return new_u, logits - lse_rows[:, None]

    specs_in = (P("dp", None), P("dp"), P("tp", None), P(None, "tp"), P(None), P(None), P(None), P(None), P(None, "tp"), P(None, "tp"), P(None, "tp"), P("tp", None))
    specs_out = (P("dp", None), P("dp", "tp"))
    return jax.shard_map(draft_step, mesh=mesh, in_specs=specs_in, out_specs=specs_out, check_vma=False)
```

```python
import functools

import jax
import jax.numpy as jnp
from jax import lax
from jax.experimental import pallas as pl
from jax.experimental.pallas import tpu as pltpu
from jax.sharding import PartitionSpec as P

NORM_EPS = 1e-6
BF16 = jnp.bfloat16
F32 = jnp.float32
GROUP_ROWS = 256
KERNEL_VMEM = 46 << 20
CORES = 2
SEND_R, SEND_L, FROM_L, FROM_R = range(4)
E_RS, E_AG, P_AG, D_RS, U_AG = range(5)


def norm_rows(values, gain):
    wide = values.astype(F32)
    inv = lax.rsqrt(jnp.mean(wide * wide, axis=-1, keepdims=True) + NORM_EPS)
    return wide * inv * gain


def norm_into(load, store, gain, n_rows, unit=16, width=4):
    width = min(width, n_rows // unit)

    @pl.loop(0, n_rows // (unit * width))
    def _(i):
        rows = [pl.ds(pl.multiple_of((i * width + u) * unit, unit), unit) for u in range(width)]
        scales = []
        for r in rows:
            wide = load(r).astype(F32)
            scales.append(lax.rsqrt(jnp.mean(wide * wide, axis=-1, keepdims=True) + NORM_EPS))
        for r, inv in zip(rows, scales):
            store(r, (load(r).astype(F32) * inv * gain[...]).astype(BF16))


def columns_of(row, lanes):
    return jnp.broadcast_to(row, (lanes, lanes)).T


def aligned(index, size):
    return pl.ds(pl.multiple_of(index * size, size), size)


def tile_of(width, most):
    return min(width, most)


def step_kernel(
    n_tp, tok, hg, eg, fg, og, hid_h, emb_h, head_h, pw_h, wg_h, wu_h, wd_h,
    pu, zst, lse,
    big, hid, land, ebuf, pbuf, pw, wg, wu, wd, erl, err, drl, drr,
    onehot, ids_ref, mst, sst, stats,
    ring, xsend, xrecv, wsend, wrecv, ssend, srecv, lsem, bsem, hsem,
):
    groups, half_rows, dim = hid.shape
    chips = n_tp // CORES
    hops = chips // 2
    rows = CORES * half_rows
    blk = half_rows // chips
    hcol = dim // 2
    hrow = half_rows // 2
    pcols = pw.shape[1] // CORES
    fcols = wg.shape[1] // CORES
    vocab = zst.shape[2]
    lanes = stats.shape[3]
    part = zst.at[:, pl.ds(0, half_rows), pl.ds(0, dim)]
    width = wg.shape[1]
    nbuf = onehot.at[pl.ds(0, half_rows), pl.ds(0, dim)]
    abuf = onehot.at[pl.ds(half_rows, half_rows), pl.ds(0, width)]
    obuf = onehot.at[:, pl.ds(0, dim)]
    q = big.shape[1]
    n_vq, n_dq = vocab // q, dim // q

    me = lax.axis_index("tp")
    z, k = me // CORES, lax.rem(me, CORES)
    other = 1 - k
    sib = z * CORES + other
    right = lax.rem(me + CORES, n_tp)
    left = lax.rem(me + n_tp - CORES, n_tp)

    def chip(offset):
        return lax.rem(z + offset + chips, chips)

    def remote(src, dst, ssem, rsem, dev):
        return pltpu.make_async_remote_copy(
            src_ref=src, dst_ref=dst, send_sem=ssem, recv_sem=rsem,
            device_id={"tp": dev}, device_id_type=pl.DeviceIdType.MESH,
        )

    def emb_copy(i, j):
        return pltpu.make_async_copy(
            emb_h.at[pl.ds(i * q, q), pl.ds(j * q, q)], big.at[i * n_dq + j], bsem.at[i * n_dq + j])

    def head_copy(i, j):
        return pltpu.make_async_copy(
            head_h.at[pl.ds(i * q, q), pl.ds(j * q, q)], big.at[i * n_vq + j], hsem.at[i * n_vq + j])

    def hid_copy(g):
        return pltpu.make_async_copy(
            hid_h.at[pl.ds(pl.multiple_of(g * rows + k * half_rows, half_rows), half_rows)], hid.at[g], lsem.at[4 + g])

    own_pw = pw.at[:, aligned(k, pcols)]
    own_wg = wg.at[:, aligned(k, fcols)]
    own_wu = wu.at[:, aligned(k, fcols)]
    own_wd = wd.at[aligned(k, fcols), :]
    oth_pw = pw.at[:, aligned(other, pcols)]
    oth_wg = wg.at[:, aligned(other, fcols)]
    oth_wu = wu.at[:, aligned(other, fcols)]
    oth_wd = wd.at[aligned(other, fcols), :]
    w_local = [pltpu.make_async_copy(s, d, lsem.at[i]) for i, (s, d) in enumerate(
        [(pw_h, own_pw), (wg_h, own_wg), (wu_h, own_wu), (wd_h, own_wd)])]
    w_send = [remote(r, r, wsend.at[i], wrecv.at[i], sib) for i, r in enumerate([own_pw, own_wg, own_wu, own_wd])]
    w_recv = [remote(r, r, wsend.at[i], wrecv.at[i], sib) for i, r in enumerate([oth_pw, oth_wg, oth_wu, oth_wd])]

    for i in range(n_vq):
        for j in range(n_dq):
            emb_copy(i, j).start()
    for c in w_local:
        c.start()

    @pl.loop(0, groups)
    def _(g):
        hid_copy(g).start()

    barrier = pltpu.get_barrier_semaphore()
    for d in range(1, n_tp):
        pl.semaphore_signal(barrier, inc=1, device_id={"tp": lax.rem(me + d, n_tp)}, device_id_type=pl.DeviceIdType.MESH)
    pl.semaphore_wait(barrier, n_tp - 1)

    def e_blk(g, o, h):
        cols = pl.ds(0, dim) if h is None else pl.ds(h * hcol, hcol)
        return ebuf.at[g, aligned(o, blk), cols]

    def p_blk(g, o, h):
        r = pl.ds(0, half_rows) if h is None else pl.ds(h * hrow, hrow)
        return pbuf.at[g, r, aligned(o, CORES * pcols)]

    def u_blk(g, o, h):
        cols = pl.ds(0, dim) if h is None else pl.ds(h * hcol, hcol)
        return pu.at[g, pl.ds(pl.multiple_of(k * half_rows + o * blk, blk), blk), cols]

    def ag_pair(c, block, g, s):
        last = s == hops
        r = block(g, chip(-(s - 1)), 0 if last else None)
        l = block(g, chip(s - 1), 1 if last else None)
        return (remote(r, r, ring.at[c, SEND_R, g, s - 1], ring.at[c, FROM_L, g, s - 1], right),
                remote(l, l, ring.at[c, SEND_L, g, s - 1], ring.at[c, FROM_R, g, s - 1], left))

    def ag_wait(c, block, g, s):
        last = s == hops
        r = block(g, chip(-s), 0 if last else None)
        l = block(g, chip(s), 1 if last else None)
        return (remote(r, r, ring.at[c, SEND_R, g, s - 1], ring.at[c, FROM_L, g, s - 1], right),
                remote(l, l, ring.at[c, SEND_L, g, s - 1], ring.at[c, FROM_R, g, s - 1], left))

    def ag_send(c, block, g, s):
        for cp in ag_pair(c, block, g, s):
            cp.start()

    def ag_step(c, block, g, s):
        got, send = ag_wait(c, block, g, s - 1), ag_pair(c, block, g, s)
        for a, b in zip(got, send):
            a.wait_recv()
            b.start()

    def rs_part(ref, h):
        return ref if h is None else ref.at[:, pl.ds(h * hcol, hcol)]

    def rs_pair(c, own, lands, g, s):
        out = []
        for kind, frm, side, dev, h1, sign in ((SEND_R, FROM_L, 0, right, 0, 1), (SEND_L, FROM_R, 1, left, 1, -1)):
            h = h1 if s == 1 else None
            dst = rs_part(lands[side].at[g, s - 1], h)
            src = rs_part(own.at[g, aligned(chip(sign * hops), blk)], h) if s == 1 else lands[side].at[g, s - 2]
            out.append(remote(src, dst, ring.at[c, kind, g, s - 1], ring.at[c, frm, g, s - 1], dev))
        return out

    def rs_wait(c, own, lands, g, s):
        return rs_pair(c, own, lands, g, s)

    def rs_first(c, own, lands, g):
        for cp in rs_pair(c, own, lands, g, 1):
            cp.start()

    def rs_step(c, own, lands, g, s):
        got, send = rs_wait(c, own, lands, g, s - 1), rs_pair(c, own, lands, g, s)
        for side, sign in ((0, 1), (1, -1)):
            got[side].wait_recv()
            o = aligned(chip(sign * (hops + 1 - s)), blk)
            slot = lands[side].at[g, s - 2]
            if s == 2:
                for h in range(2):
                    c_ = slice(h * hcol, (h + 1) * hcol)
                    mine = own[g, o, c_]
                    slot[:, c_] = slot[:, c_] + mine if h == side else mine
            else:
                slot[...] = slot[...] + own[g, o, :]
            send[side].start()

    def rs_sum(c, own, lands, g):
        for cp in rs_wait(c, own, lands, g, hops):
            cp.wait_recv()
        mine = own[g, aligned(z, blk), :]
        return lands[0][g, hops - 1].astype(F32) + mine.astype(F32) + lands[1][g, hops - 1].astype(F32)

    e_lands, d_lands = (erl, err), (drl, drr)

    def pick_swap(g):
        return remote(pu.at[g, aligned(other, half_rows)], land.at[g], xsend.at[0, g], xrecv.at[0, g], sib)

    def u_swap(g, c):
        r = pu.at[g, aligned(c, half_rows)]
        return remote(r, r, xsend.at[1, g], xrecv.at[1, g], sib)

    def stat_send(g, d):
        return remote(stats.at[g, me], stats.at[g, me], ssend.at[g, d], srecv.at[g, d], lax.rem(me + d, n_tp))

    def stat_wait(g, d):
        src = lax.rem(me + n_tp - d, n_tp)
        return remote(stats.at[g, src], stats.at[g, src], ssend.at[g, d], srecv.at[g, d], lax.rem(me + d, n_tp))

    def picks(g):
        @pl.when(g == 0)
        def _():
            for i in range(n_vq):
                for j in range(n_dq):
                    emb_copy(i, j).wait()

        per = rows // lanes
        for i in range(per):
            row = (tok[pl.ds(g * per + i, 1), :] - me * vocab).astype(F32)
            ids_ref[i * lanes:(i + 1) * lanes, :] = columns_of(row, lanes)
        lane = lax.broadcasted_iota(jnp.int32, (rows, lanes), 1).astype(F32)

        @pl.loop(0, vocab // lanes)
        def _(j):
            first = (j * lanes).astype(F32)
            onehot[:, aligned(j, lanes)] = jnp.where(ids_ref[...] == lane + first, 1.0, 0.0).astype(BF16)

        tn = tile_of(q, 512)
        for j in range(n_dq):
            @pl.loop(0, q // tn)
            def _(t):
                acc = None
                for i in range(n_vq):
                    d = jnp.dot(onehot[:, i * q:(i + 1) * q], big[i * n_dq + j, :, aligned(t, tn)], preferred_element_type=F32)
                    acc = d if acc is None else acc + d
                pu[g, :, pl.ds(pl.multiple_of(j * q + t * tn, tn), tn)] = acc.astype(BF16)

        pick_swap(g).start()

        @pl.when(g == groups - 1)
        def _():
            for i in range(n_dq):
                for j in range(n_vq):
                    head_copy(i, j).start()

        @pl.when(g == 0)
        def _():
            w_local[0].wait()
            w_send[0].start()

    def pick_sum(g):
        pick_swap(g).wait_recv()

        for i in range(chips):
            r = pl.ds(i * blk, blk)
            land[g, r, :] = land[g, r, :] + pu[g, pl.ds(pl.multiple_of(k * half_rows + i * blk, blk), blk), :]

        rs_first(E_RS, land, e_lands, g)

    def e_norm(g):
        pick_swap(g).wait_send()
        ebuf[g, aligned(z, blk), :] = norm_rows(rs_sum(E_RS, land, e_lands, g), eg[...]).astype(BF16)
        ag_send(E_AG, e_blk, g, 1)

    def h_norm(g):
        hid_copy(g).wait()

        def put(r, v):
            hid[g, r, :] = v

        norm_into(lambda r: hid[g, r, :], put, hg, half_rows)

        @pl.when(g == 0)
        def _():
            for i in range(1, 4):
                w_local[i].wait()
                w_send[i].start()

    def project(g):
        for cp in ag_wait(E_AG, e_blk, g, hops):
            cp.wait_recv()

        @pl.when(g == 0)
        def _():
            w_recv[0].wait_recv()

        out = jnp.dot(hid[g], pw[:dim, :], preferred_element_type=F32)
        out += jnp.dot(ebuf[g], pw[dim:, :], preferred_element_type=F32)
        pbuf[g, :, aligned(z, CORES * pcols)] = out.astype(BF16)
        ag_send(P_AG, p_blk, g, 1)

    def ffn_up(g, first):
        if first:
            for cp in ag_wait(P_AG, p_blk, g, hops):
                cp.wait_recv()

            @pl.when(g == 0)
            def _():
                for i in range(1, 4):
                    w_recv[i].wait_recv()

            def put(r, v):
                nbuf[r, :] = v

            norm_into(lambda r: pbuf[g, r, :], put, fg, half_rows)

        tn = tile_of(width, 256)
        n = width // tn
        lo, hi = (0, n // 2) if first else (n // 2, n)

        @pl.loop(lo, hi)
        def _(t):
            c = aligned(t, tn)
            gate = jnp.dot(nbuf[...], wg[:, c], preferred_element_type=F32)
            up = jnp.dot(nbuf[...], wu[:, c], preferred_element_type=F32)
            abuf[:, c] = (jax.nn.silu(gate) * up).astype(BF16)

    def ffn_down(g):
        tm = tile_of(dim, 512)

        @pl.loop(0, dim // tm)
        def _(t):
            c = aligned(t, tm)
            part[g, :, c] = jnp.dot(abuf[...], wd[:, c], preferred_element_type=F32)

        rs_first(D_RS, part, d_lands, g)

    def new_u(g):
        for cp in rs_pair(D_RS, part, d_lands, g, 1):
            cp.wait_send()
        total = rs_sum(D_RS, part, d_lands, g)
        total = pbuf[g, aligned(z, blk), :].astype(F32) + total
        pu[g, pl.ds(pl.multiple_of(k * half_rows + z * blk, blk), blk), :] = total.astype(BF16)
        ag_send(U_AG, u_blk, g, 1)

    def u_done(g):
        for cp in ag_wait(U_AG, u_blk, g, hops):
            cp.wait_recv()
        u_swap(g, k).start()

    def head(g, j):
        if j == 0:
            u_swap(g, other).wait_recv()

            @pl.when(g == 0)
            def _():
                for i in range(n_dq):
                    for jj in range(n_vq):
                        head_copy(i, jj).wait()

            def put(r, v):
                obuf[r, :] = v

            norm_into(lambda r: pu[g, r, :], put, og, rows)

        tn = tile_of(q, 512)

        @pl.loop(0, q // tn)
        def _(t):
            acc = None
            for i in range(n_dq):
                d = jnp.dot(obuf[:, i * q:(i + 1) * q], big[i * n_vq + j, :, aligned(t, tn)], preferred_element_type=F32)
                acc = d if acc is None else acc + d
            zst[g, :, pl.ds(pl.multiple_of(j * q + t * tn, tn), tn)] = acc

    def row_stats(g):
        unit, wide = 8, 8

        @pl.loop(0, rows // (unit * wide))
        def _(i):
            rr = [pl.ds(pl.multiple_of((i * wide + u) * unit, unit), unit) for u in range(wide)]
            tops = [jnp.max(zst[g, r, :], axis=-1, keepdims=True) for r in rr]
            for r, m in zip(rr, tops):
                s = jnp.sum(jnp.exp(zst[g, r, :] - m), axis=-1, keepdims=True)
                mst[r, :] = jnp.broadcast_to(m, (unit, lanes))
                sst[r, :] = jnp.broadcast_to(s, (unit, lanes))

        mt, st = mst[...].T, sst[...].T
        n = rows // lanes
        for i in range(n):
            c = slice(i * lanes, (i + 1) * lanes)
            stats[g, me, i:i + 1, :] = mt[0:1, c]
            stats[g, me, n + i:n + i + 1, :] = st[0:1, c]
        for d in range(1, n_tp):
            stat_send(g, d).start()

    def total_lse(g):
        for d in range(1, n_tp):
            stat_wait(g, d).wait_recv()
        n = rows // lanes
        ms = [stats[g, i, 0:n, :] for i in range(n_tp)]
        top = functools.reduce(jnp.maximum, ms)
        tot = functools.reduce(jnp.add, [stats[g, i, n:2 * n, :] * jnp.exp(ms[i] - top) for i in range(n_tp)])
        total = top + jnp.log(tot)
        for i in range(n):
            lse[g, i * lanes:(i + 1) * lanes, :] = columns_of(total[i:i + 1, :], lanes)

    bind = functools.partial
    stages = [[picks], [pick_sum]]
    stages += [[bind(rs_step, E_RS, land, e_lands, s=s)] for s in range(2, hops + 1)]
    stages += [[e_norm]]
    stages += [[bind(ag_step, E_AG, e_blk, s=s)] for s in range(2, hops + 1)]
    stages[-1].append(h_norm)
    stages += [[project]]
    stages += [[bind(ag_step, P_AG, p_blk, s=s)] for s in range(2, hops + 1)]
    stages += [[bind(ffn_up, first=True), bind(ffn_up, first=False), ffn_down]]
    stages += [[bind(rs_step, D_RS, part, d_lands, s=s)] for s in range(2, hops + 1)]
    stages += [[new_u]]
    stages += [[bind(ag_step, U_AG, u_blk, s=s)] for s in range(2, hops + 1)]
    stages += [[u_done]]
    stages += [[bind(head, j=j) for j in range(n_vq)] + [row_stats]]
    stages += [[total_lse]]
    order = sorted((-i + p, p > 0, i, p) for i, pieces in enumerate(stages) for p in range(len(pieces)))

    @pl.loop(0, groups + len(stages) - 1)
    def _(t):
        for _, _, i, p in order:
            g = t - i

            @pl.when((g >= 0) & (g < groups))
            def _():
                stages[i][p](g=g)

    for cp in w_send:
        cp.wait_send()

    @pl.loop(0, groups)
    def _(g):
        for s in range(1, hops + 1):
            for cp in rs_pair(E_RS, land, e_lands, g, s):
                cp.wait_send()
            if s > 1:
                for cp in rs_pair(D_RS, part, d_lands, g, s):
                    cp.wait_send()
            for c, b in ((E_AG, e_blk), (P_AG, p_blk), (U_AG, u_blk)):
                for cp in ag_pair(c, b, g, s):
                    cp.wait_send()
        u_swap(g, k).wait_send()
        for d in range(1, n_tp):
            stat_send(g, d).wait_send()


def finish_kernel(z, lse, pu, logp, u, sem):
    i = pl.program_id(0)
    n_rows, vocab = logp.shape
    unit, lanes = 16, lse.shape[1]
    u_copy = pltpu.make_async_copy(pu, u, sem)

    @pl.when(i == 0)
    def _():
        u_copy.start()

    @pl.loop(0, n_rows // unit)
    def _(c):
        r = aligned(i * (n_rows // unit) + c, unit)
        base = lse[r, :]
        for j in range(vocab // lanes):
            cols = slice(j * lanes, (j + 1) * lanes)
            logp[aligned(c, unit), cols] = z[r, cols] - base

    @pl.when(i == pl.num_programs(0) - 1)
    def _():
        u_copy.wait()


def finish_call(z, lse, pu):
    batch, vocab = z.shape
    vm = pl.BlockSpec(memory_space=pltpu.VMEM)
    step = GROUP_ROWS // CORES
    return pl.pallas_call(
        finish_kernel,
        grid=(batch // step,),
        out_shape=(jax.ShapeDtypeStruct((batch, vocab), F32), jax.ShapeDtypeStruct(pu.shape, BF16)),
        in_specs=[vm, vm, vm],
        out_specs=(pl.BlockSpec((step, vocab), lambda i: (i, 0)), pl.BlockSpec(memory_space=pltpu.HBM)),
        scratch_shapes=[pltpu.SemaphoreType.DMA],
        compiler_params=pltpu.CompilerParams(vmem_limit_bytes=6 << 20),
        name="finish",
    )(z, lse, pu)


def draft_call(n_tp, hidden, tokens, embedding, head_w, h_norm, e_norm, f_norm, o_norm, proj_w, w_gate, w_up, w_down):
    batch, dim = hidden.shape
    vocab = embedding.shape[0]
    pcols, fcols = proj_w.shape[1], w_gate.shape[1]
    groups = batch // GROUP_ROWS
    half_rows = GROUP_ROWS // CORES
    chips = n_tp // CORES
    hops = chips // 2
    blk = half_rows // chips
    q = dim // 2
    lanes = 128
    tok = tokens.reshape(batch // lanes, lanes)
    vm = pl.BlockSpec(memory_space=pltpu.VMEM)
    hbm = pl.BlockSpec(memory_space=pltpu.HBM)
    dma = pltpu.SemaphoreType.DMA
    n_big = (vocab // q) * (dim // q)
    flops = 2 * batch * (2 * dim * vocab + 2 * dim * pcols + 3 * dim * fcols)
    return pl.pallas_call(
        functools.partial(step_kernel, n_tp),
        out_shape=(
            pltpu.VMEM((groups, GROUP_ROWS, dim), BF16),
            pltpu.VMEM((groups, GROUP_ROWS, vocab), F32),
            pltpu.VMEM((groups, GROUP_ROWS, lanes), F32),
        ),
        in_specs=[vm] * 5 + [hbm] * 7,
        out_specs=(vm, vm, vm),
        scratch_shapes=[
            pltpu.VMEM((n_big, q, q), BF16),
            pltpu.VMEM((groups, half_rows, dim), BF16),
            pltpu.VMEM((groups, half_rows, dim), BF16),
            pltpu.VMEM((groups, half_rows, dim), BF16),
            pltpu.VMEM((groups, half_rows, dim), BF16),
            pltpu.VMEM((2 * dim, CORES * pcols), BF16),
            pltpu.VMEM((dim, CORES * fcols), BF16),
            pltpu.VMEM((dim, CORES * fcols), BF16),
            pltpu.VMEM((CORES * fcols, dim), BF16),
            pltpu.VMEM((groups, hops, blk, dim), BF16),
            pltpu.VMEM((groups, hops, blk, dim), BF16),
            pltpu.VMEM((groups, hops, blk, dim), F32),
            pltpu.VMEM((groups, hops, blk, dim), F32),
            pltpu.VMEM((GROUP_ROWS, vocab), BF16),
            pltpu.VMEM((GROUP_ROWS, lanes), F32),
            pltpu.VMEM((GROUP_ROWS, lanes), F32),
            pltpu.VMEM((GROUP_ROWS, lanes), F32),
            pltpu.VMEM((groups, n_tp, 8, lanes), F32),
            dma((5, 4, groups, hops)),
            dma((2, groups)),
            dma((2, groups)),
            dma((4,)),
            dma((4,)),
            dma((groups, n_tp)),
            dma((groups, n_tp)),
            dma((4 + groups,)),
            dma((n_big,)),
            dma((n_big,)),
        ],
        compiler_params=pltpu.CompilerParams(
            collective_id=0, has_side_effects=True, vmem_limit_bytes=KERNEL_VMEM),
        cost_estimate=pl.CostEstimate(flops=flops, bytes_accessed=70 << 20, transcendentals=0),
        name="draft_step",
    )(tok, h_norm[None], e_norm[None], f_norm[None], o_norm[None], hidden, embedding, head_w, proj_w, w_gate, w_up, w_down)


def solution(mesh):
    n_tp = mesh.shape["tp"]

    def draft_step(hidden, *rest):
        batch, dim = hidden.shape
        pu, z, lse = draft_call(n_tp, hidden, *rest)
        logp, new_u = finish_call(z.reshape(batch, -1), lse.reshape(batch, -1), pu.reshape(batch, dim))
        return new_u, logp

    specs_in = (P("dp", None), P("dp"), P("tp", None), P(None, "tp"), P(None), P(None), P(None), P(None), P(None, "tp"), P(None, "tp"), P(None, "tp"), P("tp", None))
    specs_out = (P("dp", None), P("dp", "tp"))
    return jax.shard_map(draft_step, mesh=mesh, in_specs=specs_in, out_specs=specs_out, check_vma=False)
```

```python
import functools

import jax
import jax.numpy as jnp
from jax import lax
from jax.experimental import pallas as pl
from jax.experimental.pallas import tpu as pltpu
from jax.sharding import PartitionSpec as P

NORM_EPS = 1e-6
BF16 = jnp.bfloat16
F32 = jnp.float32
GROUP_ROWS = 256
LOWEST = -3e38
KERNEL_VMEM = 46 << 20
CORES = 2
SEND_R, SEND_L, FROM_L, FROM_R = range(4)
E_RS, E_AG, P_AG, D_RS, U_AG = range(5)


def norm_rows(values, gain):
    wide = values.astype(F32)
    inv = lax.rsqrt(jnp.mean(wide * wide, axis=-1, keepdims=True) + NORM_EPS)
    return wide * inv * gain


def norm_into(load, store, gain, n_rows, unit=16, width=4):
    width = min(width, n_rows // unit)

    @pl.loop(0, n_rows // (unit * width))
    def _(i):
        rows = [pl.ds(pl.multiple_of((i * width + u) * unit, unit), unit) for u in range(width)]
        scales = []
        for r in rows:
            wide = load(r).astype(F32)
            scales.append(lax.rsqrt(jnp.mean(wide * wide, axis=-1, keepdims=True) + NORM_EPS))
        for r, inv in zip(rows, scales):
            store(r, (load(r).astype(F32) * inv * gain[...]).astype(BF16))


def columns_of(row, lanes):
    return jnp.broadcast_to(row, (lanes, lanes)).T


def aligned(index, size):
    return pl.ds(pl.multiple_of(index * size, size), size)


def tile_of(width, most):
    return min(width, most)


def step_kernel(
    n_tp, tok, hg, eg, fg, og, hid_h, emb_h, head_h, pw_h, wg_h, wu_h, wd_h,
    pu, zst, lse,
    big, hid, land, ebuf, pbuf, pw, wg, wu, wd, erl, err, drl, drr,
    onehot, ids_ref, mst, sst, stats,
    ring, xsend, xrecv, wsend, wrecv, ssend, srecv, lsem, bsem, hsem,
):
    groups, half_rows, dim = hid.shape
    chips = n_tp // CORES
    hops = chips // 2
    rows = CORES * half_rows
    blk = half_rows // chips
    hcol = dim // 2
    hrow = half_rows // 2
    pcols = pw.shape[1] // CORES
    fcols = wg.shape[1] // CORES
    vocab = zst.shape[2]
    lanes = stats.shape[3]
    part = zst.at[:, pl.ds(0, half_rows), pl.ds(0, dim)]
    width = wg.shape[1]
    nbuf = onehot.at[pl.ds(0, half_rows), pl.ds(0, dim)]
    abuf = onehot.at[pl.ds(half_rows, half_rows), pl.ds(0, width)]
    obuf = onehot.at[:, pl.ds(0, dim)]
    q = big.shape[1]
    n_vq, n_dq = vocab // q, dim // q

    me = lax.axis_index("tp")
    z, k = me // CORES, lax.rem(me, CORES)
    other = 1 - k
    sib = z * CORES + other
    right = lax.rem(me + CORES, n_tp)
    left = lax.rem(me + n_tp - CORES, n_tp)

    def chip(offset):
        return lax.rem(z + offset + chips, chips)

    def remote(src, dst, ssem, rsem, dev):
        return pltpu.make_async_remote_copy(
            src_ref=src, dst_ref=dst, send_sem=ssem, recv_sem=rsem,
            device_id={"tp": dev}, device_id_type=pl.DeviceIdType.MESH,
        )

    def emb_copy(i, j):
        return pltpu.make_async_copy(
            emb_h.at[pl.ds(i * q, q), pl.ds(j * q, q)], big.at[i * n_dq + j], bsem.at[i * n_dq + j])

    def head_copy(i, j):
        return pltpu.make_async_copy(
            head_h.at[pl.ds(i * q, q), pl.ds(j * q, q)], big.at[i * n_vq + j], hsem.at[i * n_vq + j])

    def hid_copy(g):
        return pltpu.make_async_copy(
            hid_h.at[pl.ds(pl.multiple_of(g * rows + k * half_rows, half_rows), half_rows)], hid.at[g], lsem.at[4 + g])

    own_pw = pw.at[:, aligned(k, pcols)]
    own_wg = wg.at[:, aligned(k, fcols)]
    own_wu = wu.at[:, aligned(k, fcols)]
    own_wd = wd.at[aligned(k, fcols), :]
    oth_pw = pw.at[:, aligned(other, pcols)]
    oth_wg = wg.at[:, aligned(other, fcols)]
    oth_wu = wu.at[:, aligned(other, fcols)]
    oth_wd = wd.at[aligned(other, fcols), :]
    w_local = [pltpu.make_async_copy(s, d, lsem.at[i]) for i, (s, d) in enumerate(
        [(pw_h, own_pw), (wg_h, own_wg), (wu_h, own_wu), (wd_h, own_wd)])]
    w_send = [remote(r, r, wsend.at[i], wrecv.at[i], sib) for i, r in enumerate([own_pw, own_wg, own_wu, own_wd])]
    w_recv = [remote(r, r, wsend.at[i], wrecv.at[i], sib) for i, r in enumerate([oth_pw, oth_wg, oth_wu, oth_wd])]

    barrier = pltpu.get_barrier_semaphore()
    for d in range(1, n_tp):
        pl.semaphore_signal(barrier, inc=1, device_id={"tp": lax.rem(me + d, n_tp)}, device_id_type=pl.DeviceIdType.MESH)
    for j in range(n_dq):
        for i in range(n_vq):
            emb_copy(i, j).start()

    def e_blk(g, o, h):
        cols = pl.ds(0, dim) if h is None else pl.ds(h * hcol, hcol)
        return ebuf.at[g, aligned(o, blk), cols]

    def p_blk(g, o, h):
        r = pl.ds(0, half_rows) if h is None else pl.ds(h * hrow, hrow)
        return pbuf.at[g, r, aligned(o, CORES * pcols)]

    def u_blk(g, o, h):
        cols = pl.ds(0, dim) if h is None else pl.ds(h * hcol, hcol)
        return pu.at[g, pl.ds(pl.multiple_of(k * half_rows + o * blk, blk), blk), cols]

    def ag_pair(c, block, g, s):
        last = s == hops
        r = block(g, chip(-(s - 1)), 0 if last else None)
        l = block(g, chip(s - 1), 1 if last else None)
        return (remote(r, r, ring.at[c, SEND_R, g, s - 1], ring.at[c, FROM_L, g, s - 1], right),
                remote(l, l, ring.at[c, SEND_L, g, s - 1], ring.at[c, FROM_R, g, s - 1], left))

    def ag_wait(c, block, g, s):
        last = s == hops
        r = block(g, chip(-s), 0 if last else None)
        l = block(g, chip(s), 1 if last else None)
        return (remote(r, r, ring.at[c, SEND_R, g, s - 1], ring.at[c, FROM_L, g, s - 1], right),
                remote(l, l, ring.at[c, SEND_L, g, s - 1], ring.at[c, FROM_R, g, s - 1], left))

    def ag_send(c, block, g, s):
        for cp in ag_pair(c, block, g, s):
            cp.start()

    def ag_step(c, block, g, s):
        got, send = ag_wait(c, block, g, s - 1), ag_pair(c, block, g, s)
        for a, b in zip(got, send):
            a.wait_recv()
            b.start()

    def rs_part(ref, h):
        return ref if h is None else ref.at[:, pl.ds(h * hcol, hcol)]

    def rs_pair(c, own, lands, g, s):
        out = []
        for kind, frm, side, dev, h1, sign in ((SEND_R, FROM_L, 0, right, 0, 1), (SEND_L, FROM_R, 1, left, 1, -1)):
            h = h1 if s == 1 else None
            dst = rs_part(lands[side].at[g, s - 1], h)
            src = rs_part(own.at[g, aligned(chip(sign * hops), blk)], h) if s == 1 else lands[side].at[g, s - 2]
            out.append(remote(src, dst, ring.at[c, kind, g, s - 1], ring.at[c, frm, g, s - 1], dev))
        return out

    def rs_wait(c, own, lands, g, s):
        return rs_pair(c, own, lands, g, s)

    def rs_first(c, own, lands, g):
        for cp in rs_pair(c, own, lands, g, 1):
            cp.start()

    def rs_step(c, own, lands, g, s):
        got, send = rs_wait(c, own, lands, g, s - 1), rs_pair(c, own, lands, g, s)
        for side, sign in ((0, 1), (1, -1)):
            got[side].wait_recv()
            o = aligned(chip(sign * (hops + 1 - s)), blk)
            slot = lands[side].at[g, s - 2]
            if s == 2:
                for h in range(2):
                    c_ = slice(h * hcol, (h + 1) * hcol)
                    mine = own[g, o, c_]
                    slot[:, c_] = slot[:, c_] + mine if h == side else mine
            else:
                slot[...] = slot[...] + own[g, o, :]
            send[side].start()

    def rs_sum(c, own, lands, g):
        for cp in rs_wait(c, own, lands, g, hops):
            cp.wait_recv()
        mine = own[g, aligned(z, blk), :]
        return lands[0][g, hops - 1].astype(F32) + mine.astype(F32) + lands[1][g, hops - 1].astype(F32)

    e_lands, d_lands = (erl, err), (drl, drr)

    def pick_swap(g):
        return remote(pu.at[g, aligned(other, half_rows)], land.at[g], xsend.at[0, g], xrecv.at[0, g], sib)

    def u_swap(g, c):
        r = pu.at[g, aligned(c, half_rows)]
        return remote(r, r, xsend.at[1, g], xrecv.at[1, g], sib)

    def stat_send(g, d):
        return remote(stats.at[g, me], stats.at[g, me], ssend.at[g, d], srecv.at[g, d], lax.rem(me + d, n_tp))

    def stat_wait(g, d):
        src = lax.rem(me + n_tp - d, n_tp)
        return remote(stats.at[g, src], stats.at[g, src], ssend.at[g, d], srecv.at[g, d], lax.rem(me + d, n_tp))

    def one_hot(g):
        per = rows // lanes
        for i in range(per):
            row = (tok[pl.ds(g * per + i, 1), :] - me * vocab).astype(F32)
            ids_ref[i * lanes:(i + 1) * lanes, :] = columns_of(row, lanes)
        lane = lax.broadcasted_iota(jnp.int32, (rows, lanes), 1)

        @pl.loop(0, vocab // lanes, unroll=4)
        def _(j):
            here = (lane + j * lanes).astype(F32)
            onehot[:, aligned(j, lanes)] = jnp.where(ids_ref[...] == here, 1.0, 0.0).astype(BF16)

    def pick_cols(g, j):
        tn = tile_of(q, 512)

        @pl.loop(0, q // tn)
        def _(t):
            acc = None
            for i in range(n_vq):
                d = jnp.dot(onehot[:, i * q:(i + 1) * q], big[i * n_dq + j, :, aligned(t, tn)], preferred_element_type=F32)
                acc = d if acc is None else acc + d
            pu[g, :, pl.ds(pl.multiple_of(j * q + t * tn, tn), tn)] = acc.astype(BF16)

    def picks(g, j):
        @pl.when(g > 0)
        def _():
            if j == 0:
                one_hot(g)
            pick_cols(g, j)
            if j == n_dq - 1:
                pick_swap(g).start()

        if j == n_dq - 1:
            @pl.when(g == groups - 1)
            def _():
                for i in range(n_dq):
                    for jj in range(n_vq):
                        head_copy(i, jj).start()

    def pick_sum(g):
        pick_swap(g).wait_recv()

        for i in range(chips):
            r = pl.ds(i * blk, blk)
            land[g, r, :] = land[g, r, :] + pu[g, pl.ds(pl.multiple_of(k * half_rows + i * blk, blk), blk), :]

        rs_first(E_RS, land, e_lands, g)

    def e_norm(g):
        pick_swap(g).wait_send()
        ebuf[g, aligned(z, blk), :] = norm_rows(rs_sum(E_RS, land, e_lands, g), eg[...]).astype(BF16)
        ag_send(E_AG, e_blk, g, 1)

    def h_norm(g):
        hid_copy(g).wait()

        def put(r, v):
            hid[g, r, :] = v

        norm_into(lambda r: hid[g, r, :], put, hg, half_rows)

        @pl.when(g == 0)
        def _():
            for i in range(1, 4):
                w_local[i].wait()
                w_send[i].start()

    def project(g):
        for cp in ag_wait(E_AG, e_blk, g, hops):
            cp.wait_recv()

        @pl.when(g == 0)
        def _():
            w_recv[0].wait_recv()

        out = jnp.dot(hid[g], pw[:dim, :], preferred_element_type=F32)
        out += jnp.dot(ebuf[g], pw[dim:, :], preferred_element_type=F32)
        pbuf[g, :, aligned(z, CORES * pcols)] = out.astype(BF16)
        ag_send(P_AG, p_blk, g, 1)

    def ffn_up(g, first):
        if first:
            for cp in ag_wait(P_AG, p_blk, g, hops):
                cp.wait_recv()

            @pl.when(g == 0)
            def _():
                for i in range(1, 4):
                    w_recv[i].wait_recv()

            def put(r, v):
                nbuf[r, :] = v

            norm_into(lambda r: pbuf[g, r, :], put, fg, half_rows)

        tn = tile_of(width, 256)
        n = width // tn
        lo, hi = (0, n // 2) if first else (n // 2, n)

        @pl.loop(lo, hi)
        def _(t):
            c = aligned(t, tn)
            gate = jnp.dot(nbuf[...], wg[:, c], preferred_element_type=F32)
            up = jnp.dot(nbuf[...], wu[:, c], preferred_element_type=F32)
            abuf[:, c] = (jax.nn.silu(gate) * up).astype(BF16)

    def ffn_down(g):
        tm = tile_of(dim, 512)

        @pl.loop(0, dim // tm)
        def _(t):
            c = aligned(t, tm)
            part[g, :, c] = jnp.dot(abuf[...], wd[:, c], preferred_element_type=F32)

        rs_first(D_RS, part, d_lands, g)

    def new_u(g):
        for cp in rs_pair(D_RS, part, d_lands, g, 1):
            cp.wait_send()
        total = rs_sum(D_RS, part, d_lands, g)
        total = pbuf[g, aligned(z, blk), :].astype(F32) + total
        pu[g, pl.ds(pl.multiple_of(k * half_rows + z * blk, blk), blk), :] = total.astype(BF16)
        ag_send(U_AG, u_blk, g, 1)

    def u_done(g):
        for cp in ag_wait(U_AG, u_blk, g, hops):
            cp.wait_recv()
        u_swap(g, k).start()

    def lane_stats(g, first, n):
        unit = 16

        @pl.loop(0, rows // unit, unroll=2)
        def _(i):
            r = aligned(i, unit)
            parts = [zst[g, r, pl.ds(pl.multiple_of(first + b * lanes, lanes), lanes)] for b in range(n // lanes)]
            old = mst[r, :]
            top = functools.reduce(jnp.maximum, parts, old)
            total = sst[r, :] * jnp.exp(old - top)
            for v in parts:
                total += jnp.exp(v - top)
            mst[r, :] = top
            sst[r, :] = total

    def head(g, j):
        tn = tile_of(q, 512)
        if j == 0:
            u_swap(g, other).wait_recv()

            @pl.when(g == 0)
            def _():
                for i in range(n_dq):
                    for jj in range(n_vq):
                        head_copy(i, jj).wait()

            def put(r, v):
                obuf[r, :] = v

            norm_into(lambda r: pu[g, r, :], put, og, rows)
            mst[...] = jnp.full(mst.shape, LOWEST, F32)
            sst[...] = jnp.zeros(sst.shape, F32)

        @pl.loop(0, q // tn)
        def _(t):
            acc = None
            for i in range(n_dq):
                d = jnp.dot(obuf[:, i * q:(i + 1) * q], big[i * n_vq + j, :, aligned(t, tn)], preferred_element_type=F32)
                acc = d if acc is None else acc + d
            zst[g, :, pl.ds(pl.multiple_of(j * q + t * tn, tn), tn)] = acc
            lane_stats(g, j * q + t * tn, tn)

    def row_stats(g):
        m = mst[...]
        top = jnp.max(m, axis=-1, keepdims=True)
        s = jnp.sum(sst[...] * jnp.exp(m - top), axis=-1, keepdims=True)
        mt = jnp.broadcast_to(top, mst.shape).T
        st = jnp.broadcast_to(s, sst.shape).T
        n = rows // lanes
        for i in range(n):
            c = slice(i * lanes, (i + 1) * lanes)
            stats[g, me, i:i + 1, :] = mt[0:1, c]
            stats[g, me, n + i:n + i + 1, :] = st[0:1, c]
        for d in range(1, n_tp):
            stat_send(g, d).start()

    def total_lse(g):
        for d in range(1, n_tp):
            stat_wait(g, d).wait_recv()
        n = rows // lanes
        ms = [stats[g, i, 0:n, :] for i in range(n_tp)]
        top = functools.reduce(jnp.maximum, ms)
        tot = functools.reduce(jnp.add, [stats[g, i, n:2 * n, :] * jnp.exp(ms[i] - top) for i in range(n_tp)])
        total = top + jnp.log(tot)
        for i in range(n):
            lse[g, i * lanes:(i + 1) * lanes, :] = columns_of(total[i:i + 1, :], lanes)

    bind = functools.partial
    stages = [[bind(picks, j=j) for j in range(n_dq)], [pick_sum]]
    stages += [[bind(rs_step, E_RS, land, e_lands, s=s)] for s in range(2, hops + 1)]
    stages += [[e_norm]]
    stages += [[bind(ag_step, E_AG, e_blk, s=s)] for s in range(2, hops + 1)]
    stages[-1].append(h_norm)
    stages += [[project]]
    stages += [[bind(ag_step, P_AG, p_blk, s=s)] for s in range(2, hops + 1)]
    stages += [[bind(ffn_up, first=True), bind(ffn_up, first=False), ffn_down]]
    stages += [[bind(rs_step, D_RS, part, d_lands, s=s)] for s in range(2, hops + 1)]
    stages += [[new_u]]
    stages += [[bind(ag_step, U_AG, u_blk, s=s)] for s in range(2, hops + 1)]
    stages += [[u_done]]
    stages += [[bind(head, j=j) for j in range(n_vq)] + [row_stats]]
    stages += [[total_lse]]
    last = len(stages) - 1
    order = []
    for i, pieces in enumerate(stages):
        for p in range(len(pieces)):
            place = (1.0 if i == last else -1.5 if (i, p) == (0, 0) else -i + p * 1.0, p > 0)
            order.append((place, i, p))
    order.sort()

    one_hot(0)
    for j in range(n_dq):
        for i in range(n_vq):
            emb_copy(i, j).wait()
        if j == n_dq - 1:
            for c in w_local:
                c.start()

            @pl.loop(0, groups)
            def _(g):
                hid_copy(g).start()

        pick_cols(0, j)
    pl.semaphore_wait(barrier, n_tp - 1)
    pick_swap(0).start()
    w_local[0].wait()
    w_send[0].start()

    @pl.loop(1, groups + last)
    def _(t):
        for _, i, p in order:
            g = t - i

            @pl.when((g >= 0) & (g < groups))
            def _():
                stages[i][p](g=g)

    for cp in w_send:
        cp.wait_send()

    @pl.loop(0, groups)
    def _(g):
        for s in range(1, hops + 1):
            for cp in rs_pair(E_RS, land, e_lands, g, s):
                cp.wait_send()
            if s > 1:
                for cp in rs_pair(D_RS, part, d_lands, g, s):
                    cp.wait_send()
            for c, b in ((E_AG, e_blk), (P_AG, p_blk), (U_AG, u_blk)):
                for cp in ag_pair(c, b, g, s):
                    cp.wait_send()
        u_swap(g, k).wait_send()
        for d in range(1, n_tp):
            stat_send(g, d).wait_send()


def finish_kernel(z, lse, pu, logp, u, sem):
    i = pl.program_id(0)
    n_rows, vocab = logp.shape
    unit, lanes = 16, lse.shape[1]
    u_copy = pltpu.make_async_copy(pu, u, sem)

    @pl.when(i == 0)
    def _():
        u_copy.start()

    @pl.loop(0, n_rows // unit)
    def _(c):
        r = aligned(i * (n_rows // unit) + c, unit)
        base = lse[r, :]
        for j in range(vocab // lanes):
            cols = slice(j * lanes, (j + 1) * lanes)
            logp[aligned(c, unit), cols] = z[r, cols] - base

    @pl.when(i == pl.num_programs(0) - 1)
    def _():
        u_copy.wait()


def finish_call(z, lse, pu):
    batch, vocab = z.shape
    vm = pl.BlockSpec(memory_space=pltpu.VMEM)
    step = GROUP_ROWS
    return pl.pallas_call(
        finish_kernel,
        grid=(batch // step,),
        out_shape=(jax.ShapeDtypeStruct((batch, vocab), F32), jax.ShapeDtypeStruct(pu.shape, BF16)),
        in_specs=[vm, vm, vm],
        out_specs=(pl.BlockSpec((step, vocab), lambda i: (i, 0)), pl.BlockSpec(memory_space=pltpu.HBM)),
        scratch_shapes=[pltpu.SemaphoreType.DMA],
        compiler_params=pltpu.CompilerParams(vmem_limit_bytes=16 << 20),
        name="finish",
    )(z, lse, pu)


def draft_call(n_tp, hidden, tokens, embedding, head_w, h_norm, e_norm, f_norm, o_norm, proj_w, w_gate, w_up, w_down):
    batch, dim = hidden.shape
    vocab = embedding.shape[0]
    pcols, fcols = proj_w.shape[1], w_gate.shape[1]
    groups = batch // GROUP_ROWS
    half_rows = GROUP_ROWS // CORES
    chips = n_tp // CORES
    hops = chips // 2
    blk = half_rows // chips
    q = dim // 2
    lanes = 128
    tok = tokens.reshape(batch // lanes, lanes)
    vm = pl.BlockSpec(memory_space=pltpu.VMEM)
    hbm = pl.BlockSpec(memory_space=pltpu.HBM)
    dma = pltpu.SemaphoreType.DMA
    n_big = (vocab // q) * (dim // q)
    flops = 2 * batch * (2 * dim * vocab + 2 * dim * pcols + 3 * dim * fcols)
    return pl.pallas_call(
        functools.partial(step_kernel, n_tp),
        out_shape=(
            pltpu.VMEM((groups, GROUP_ROWS, dim), BF16),
            pltpu.VMEM((groups, GROUP_ROWS, vocab), F32),
            pltpu.VMEM((groups, GROUP_ROWS, lanes), F32),
        ),
        in_specs=[vm] * 5 + [hbm] * 7,
        out_specs=(vm, vm, vm),
        scratch_shapes=[
            pltpu.VMEM((n_big, q, q), BF16),
            pltpu.VMEM((groups, half_rows, dim), BF16),
            pltpu.VMEM((groups, half_rows, dim), BF16),
            pltpu.VMEM((groups, half_rows, dim), BF16),
            pltpu.VMEM((groups, half_rows, dim), BF16),
            pltpu.VMEM((2 * dim, CORES * pcols), BF16),
            pltpu.VMEM((dim, CORES * fcols), BF16),
            pltpu.VMEM((dim, CORES * fcols), BF16),
            pltpu.VMEM((CORES * fcols, dim), BF16),
            pltpu.VMEM((groups, hops, blk, dim), BF16),
            pltpu.VMEM((groups, hops, blk, dim), BF16),
            pltpu.VMEM((groups, hops, blk, dim), F32),
            pltpu.VMEM((groups, hops, blk, dim), F32),
            pltpu.VMEM((GROUP_ROWS, vocab), BF16),
            pltpu.VMEM((GROUP_ROWS, lanes), F32),
            pltpu.VMEM((GROUP_ROWS, lanes), F32),
            pltpu.VMEM((GROUP_ROWS, lanes), F32),
            pltpu.VMEM((groups, n_tp, 8, lanes), F32),
            dma((5, 4, groups, hops)),
            dma((2, groups)),
            dma((2, groups)),
            dma((4,)),
            dma((4,)),
            dma((groups, n_tp)),
            dma((groups, n_tp)),
            dma((4 + groups,)),
            dma((n_big,)),
            dma((n_big,)),
        ],
        compiler_params=pltpu.CompilerParams(
            collective_id=0, has_side_effects=True, vmem_limit_bytes=KERNEL_VMEM),
        cost_estimate=pl.CostEstimate(flops=flops, bytes_accessed=70 << 20, transcendentals=0),
        name="draft_step",
    )(tok, h_norm[None], e_norm[None], f_norm[None], o_norm[None], hidden, embedding, head_w, proj_w, w_gate, w_up, w_down)


def solution(mesh):
    n_tp = mesh.shape["tp"]

    def draft_step(hidden, *rest):
        batch, dim = hidden.shape
        pu, z, lse = draft_call(n_tp, hidden, *rest)
        logp, new_u = finish_call(z.reshape(batch, -1), lse.reshape(batch, -1), pu.reshape(batch, dim))
        return new_u, logp

    specs_in = (P("dp", None), P("dp"), P("tp", None), P(None, "tp"), P(None), P(None), P(None), P(None), P(None, "tp"), P(None, "tp"), P(None, "tp"), P("tp", None))
    specs_out = (P("dp", None), P("dp", "tp"))
    return jax.shard_map(draft_step, mesh=mesh, in_specs=specs_in, out_specs=specs_out, check_vma=False)
```

```python
import functools

import jax
import jax.numpy as jnp
from jax import lax
from jax.experimental import pallas as pl
from jax.experimental.pallas import tpu as pltpu
from jax.sharding import PartitionSpec as P

NORM_EPS = 1e-6
BF16 = jnp.bfloat16
F32 = jnp.float32
GROUP_ROWS = 256
KERNEL_VMEM = 46 << 20
CORES = 2
SEND_R, SEND_L, FROM_L, FROM_R = range(4)
E_RS, E_AG, P_AG, D_RS, U_AG = range(5)


def norm_rows(values, gain):
    wide = values.astype(F32)
    inv = lax.rsqrt(jnp.mean(wide * wide, axis=-1, keepdims=True) + NORM_EPS)
    return wide * inv * gain


def norm_into(load, store, gain, n_rows, unit=16, width=4):
    width = min(width, n_rows // unit)

    @pl.loop(0, n_rows // (unit * width))
    def _(i):
        rows = [pl.ds(pl.multiple_of((i * width + u) * unit, unit), unit) for u in range(width)]
        scales = []
        for r in rows:
            wide = load(r).astype(F32)
            scales.append(lax.rsqrt(jnp.mean(wide * wide, axis=-1, keepdims=True) + NORM_EPS))
        for r, inv in zip(rows, scales):
            store(r, (load(r).astype(F32) * inv * gain[...]).astype(BF16))


def columns_of(row, lanes):
    return jnp.broadcast_to(row, (lanes, lanes)).T


def aligned(index, size):
    return pl.ds(pl.multiple_of(index * size, size), size)


def tile_of(width, most):
    return min(width, most)


def step_kernel(
    n_tp, tok, hg, eg, fg, og, hid_h, emb_h, head_h, pw_h, wg_h, wu_h, wd_h,
    pu, zst, lse,
    big, hid, land, ebuf, pbuf, pw, wg, wu, wd, erl, err, drl, drr,
    onehot, ids_ref, mst, sst, stats,
    ring, xsend, xrecv, wsend, wrecv, ssend, srecv, lsem, bsem, hsem,
):
    groups, half_rows, dim = hid.shape
    chips = n_tp // CORES
    hops = chips // 2
    rows = CORES * half_rows
    blk = half_rows // chips
    hcol = dim // 2
    hrow = half_rows // 2
    pcols = pw.shape[1] // CORES
    fcols = wg.shape[1] // CORES
    vocab = zst.shape[2]
    lanes = stats.shape[3]
    part = zst.at[:, pl.ds(0, half_rows), pl.ds(0, dim)]
    width = wg.shape[1]
    nbuf = onehot.at[pl.ds(0, half_rows), pl.ds(0, dim)]
    abuf = onehot.at[pl.ds(half_rows, half_rows), pl.ds(0, width)]
    obuf = onehot.at[:, pl.ds(0, dim)]
    q = big.shape[1]
    n_vq, n_dq = vocab // q, dim // q

    me = lax.axis_index("tp")
    z, k = me // CORES, lax.rem(me, CORES)
    other = 1 - k
    sib = z * CORES + other
    right = lax.rem(me + CORES, n_tp)
    left = lax.rem(me + n_tp - CORES, n_tp)

    def chip(offset):
        return lax.rem(z + offset + chips, chips)

    def remote(src, dst, ssem, rsem, dev):
        return pltpu.make_async_remote_copy(
            src_ref=src, dst_ref=dst, send_sem=ssem, recv_sem=rsem,
            device_id={"tp": dev}, device_id_type=pl.DeviceIdType.MESH,
        )

    def emb_copy(i, j):
        return pltpu.make_async_copy(
            emb_h.at[pl.ds(i * q, q), pl.ds(j * q, q)], big.at[j * n_vq + i], bsem.at[j * n_vq + i])

    def head_copy(i, j):
        return pltpu.make_async_copy(
            head_h.at[pl.ds(i * q, q), pl.ds(j * q, q)], big.at[j * n_dq + i], hsem.at[j * n_dq + i])

    def hid_copy(g):
        return pltpu.make_async_copy(
            hid_h.at[pl.ds(pl.multiple_of(g * rows + k * half_rows, half_rows), half_rows)], hid.at[g], lsem.at[4 + g])

    own_pw = pw.at[:, aligned(k, pcols)]
    own_wg = wg.at[:, aligned(k, fcols)]
    own_wu = wu.at[:, aligned(k, fcols)]
    own_wd = wd.at[aligned(k, fcols), :]
    oth_pw = pw.at[:, aligned(other, pcols)]
    oth_wg = wg.at[:, aligned(other, fcols)]
    oth_wu = wu.at[:, aligned(other, fcols)]
    oth_wd = wd.at[aligned(other, fcols), :]
    w_local = [pltpu.make_async_copy(s, d, lsem.at[i]) for i, (s, d) in enumerate(
        [(pw_h, own_pw), (wg_h, own_wg), (wu_h, own_wu), (wd_h, own_wd)])]
    w_send = [remote(r, r, wsend.at[i], wrecv.at[i], sib) for i, r in enumerate([own_pw, own_wg, own_wu, own_wd])]
    w_recv = [remote(r, r, wsend.at[i], wrecv.at[i], sib) for i, r in enumerate([oth_pw, oth_wg, oth_wu, oth_wd])]

    barrier = pltpu.get_barrier_semaphore()
    for d in range(1, n_tp):
        pl.semaphore_signal(barrier, inc=1, device_id={"tp": lax.rem(me + d, n_tp)}, device_id_type=pl.DeviceIdType.MESH)
    for j in range(n_dq):
        for i in range(n_vq):
            emb_copy(i, j).start()

    def e_blk(g, o, h):
        cols = pl.ds(0, dim) if h is None else pl.ds(h * hcol, hcol)
        return ebuf.at[g, aligned(o, blk), cols]

    def p_blk(g, o, h):
        r = pl.ds(0, half_rows) if h is None else pl.ds(h * hrow, hrow)
        return pbuf.at[g, r, aligned(o, CORES * pcols)]

    def u_blk(g, o, h):
        cols = pl.ds(0, dim) if h is None else pl.ds(h * hcol, hcol)
        return pu.at[g, pl.ds(pl.multiple_of(k * half_rows + o * blk, blk), blk), cols]

    def ag_pair(c, block, g, s):
        last = s == hops
        r = block(g, chip(-(s - 1)), 0 if last else None)
        l = block(g, chip(s - 1), 1 if last else None)
        return (remote(r, r, ring.at[c, SEND_R, g, s - 1], ring.at[c, FROM_L, g, s - 1], right),
                remote(l, l, ring.at[c, SEND_L, g, s - 1], ring.at[c, FROM_R, g, s - 1], left))

    def ag_wait(c, block, g, s):
        last = s == hops
        r = block(g, chip(-s), 0 if last else None)
        l = block(g, chip(s), 1 if last else None)
        return (remote(r, r, ring.at[c, SEND_R, g, s - 1], ring.at[c, FROM_L, g, s - 1], right),
                remote(l, l, ring.at[c, SEND_L, g, s - 1], ring.at[c, FROM_R, g, s - 1], left))

    def ag_send(c, block, g, s):
        for cp in ag_pair(c, block, g, s):
            cp.start()

    def ag_step(c, block, g, s):
        got, send = ag_wait(c, block, g, s - 1), ag_pair(c, block, g, s)
        for a, b in zip(got, send):
            a.wait_recv()
            b.start()

    def rs_part(ref, h):
        return ref if h is None else ref.at[:, pl.ds(h * hcol, hcol)]

    def rs_pair(c, own, lands, g, s):
        out = []
        for kind, frm, side, dev, h1, sign in ((SEND_R, FROM_L, 0, right, 0, 1), (SEND_L, FROM_R, 1, left, 1, -1)):
            h = h1 if s == 1 else None
            dst = rs_part(lands[side].at[g, s - 1], h)
            src = rs_part(own.at[g, aligned(chip(sign * hops), blk)], h) if s == 1 else lands[side].at[g, s - 2]
            out.append(remote(src, dst, ring.at[c, kind, g, s - 1], ring.at[c, frm, g, s - 1], dev))
        return out

    def rs_wait(c, own, lands, g, s):
        return rs_pair(c, own, lands, g, s)

    def rs_first(c, own, lands, g):
        for cp in rs_pair(c, own, lands, g, 1):
            cp.start()

    def rs_step(c, own, lands, g, s):
        got, send = rs_wait(c, own, lands, g, s - 1), rs_pair(c, own, lands, g, s)
        for side, sign in ((0, 1), (1, -1)):
            got[side].wait_recv()
            o = aligned(chip(sign * (hops + 1 - s)), blk)
            slot = lands[side].at[g, s - 2]
            if s == 2:
                for h in range(2):
                    c_ = slice(h * hcol, (h + 1) * hcol)
                    mine = own[g, o, c_]
                    slot[:, c_] = slot[:, c_] + mine if h == side else mine
            else:
                slot[...] = slot[...] + own[g, o, :]
            send[side].start()

    def rs_sum(c, own, lands, g):
        for cp in rs_wait(c, own, lands, g, hops):
            cp.wait_recv()
        mine = own[g, aligned(z, blk), :]
        return lands[0][g, hops - 1].astype(F32) + mine.astype(F32) + lands[1][g, hops - 1].astype(F32)

    e_lands, d_lands = (erl, err), (drl, drr)

    def pick_swap(g):
        return remote(pu.at[g, aligned(other, half_rows)], land.at[g], xsend.at[0, g], xrecv.at[0, g], sib)

    def u_swap(g, c):
        r = pu.at[g, aligned(c, half_rows)]
        return remote(r, r, xsend.at[1, g], xrecv.at[1, g], sib)

    def stat_send(g, d):
        return remote(stats.at[g, me], stats.at[g, me], ssend.at[g, d], srecv.at[g, d], lax.rem(me + d, n_tp))

    def stat_wait(g, d):
        src = lax.rem(me + n_tp - d, n_tp)
        return remote(stats.at[g, src], stats.at[g, src], ssend.at[g, d], srecv.at[g, d], lax.rem(me + d, n_tp))

    def one_hot(g):
        per = rows // lanes
        for i in range(per):
            row = (tok[pl.ds(g * per + i, 1), :] - me * vocab).astype(F32)
            ids_ref[i * lanes:(i + 1) * lanes, :] = columns_of(row, lanes)
        lane = lax.broadcasted_iota(jnp.int32, (rows, lanes), 1)

        @pl.loop(0, vocab // lanes, unroll=4)
        def _(j):
            here = (lane + j * lanes).astype(F32)
            onehot[:, aligned(j, lanes)] = jnp.where(ids_ref[...] == here, 1.0, 0.0).astype(BF16)

    def pick_cols(g, j):
        tn = tile_of(q, 1024)

        @pl.loop(0, q // tn)
        def _(t):
            table = big[j * n_vq:(j + 1) * n_vq, :, aligned(t, tn)].reshape(vocab, tn)
            acc = jnp.dot(onehot[...], table, preferred_element_type=F32)
            pu[g, :, pl.ds(pl.multiple_of(j * q + t * tn, tn), tn)] = acc.astype(BF16)

    def picks(g, j):
        @pl.when(g > 0)
        def _():
            if j == 0:
                one_hot(g)
            pick_cols(g, j)
            if j == n_dq - 1:
                pick_swap(g).start()

        if j == n_dq - 1:
            @pl.when(g == groups - 1)
            def _():
                for i in range(n_dq):
                    for jj in range(n_vq):
                        head_copy(i, jj).start()

    def pick_sum(g):
        pick_swap(g).wait_recv()

        for i in range(chips):
            r = pl.ds(i * blk, blk)
            land[g, r, :] = land[g, r, :] + pu[g, pl.ds(pl.multiple_of(k * half_rows + i * blk, blk), blk), :]

        rs_first(E_RS, land, e_lands, g)

    def e_norm(g):
        pick_swap(g).wait_send()
        ebuf[g, aligned(z, blk), :] = norm_rows(rs_sum(E_RS, land, e_lands, g), eg[...]).astype(BF16)
        ag_send(E_AG, e_blk, g, 1)

    def h_norm(g):
        hid_copy(g).wait()

        def put(r, v):
            hid[g, r, :] = v

        norm_into(lambda r: hid[g, r, :], put, hg, half_rows)

        @pl.when(g == 0)
        def _():
            for i in range(1, 4):
                w_local[i].wait()
                w_send[i].start()

    def project(g):
        for cp in ag_wait(E_AG, e_blk, g, hops):
            cp.wait_recv()

        @pl.when(g == 0)
        def _():
            w_recv[0].wait_recv()

        out = jnp.dot(hid[g], pw[:dim, :], preferred_element_type=F32)
        out += jnp.dot(ebuf[g], pw[dim:, :], preferred_element_type=F32)
        pbuf[g, :, aligned(z, CORES * pcols)] = out.astype(BF16)
        ag_send(P_AG, p_blk, g, 1)

    def ffn_up(g, first):
        if first:
            for cp in ag_wait(P_AG, p_blk, g, hops):
                cp.wait_recv()

            @pl.when(g == 0)
            def _():
                for i in range(1, 4):
                    w_recv[i].wait_recv()

            def put(r, v):
                nbuf[r, :] = v

            norm_into(lambda r: pbuf[g, r, :], put, fg, half_rows)

        tn = tile_of(width, 256)
        n = width // tn
        lo, hi = (0, n // 2) if first else (n // 2, n)

        @pl.loop(lo, hi)
        def _(t):
            c = aligned(t, tn)
            gate = jnp.dot(nbuf[...], wg[:, c], preferred_element_type=F32)
            up = jnp.dot(nbuf[...], wu[:, c], preferred_element_type=F32)
            abuf[:, c] = (jax.nn.silu(gate) * up).astype(BF16)

    def ffn_down(g):
        tm = tile_of(dim, 512)

        @pl.loop(0, dim // tm)
        def _(t):
            c = aligned(t, tm)
            part[g, :, c] = jnp.dot(abuf[...], wd[:, c], preferred_element_type=F32)

        rs_first(D_RS, part, d_lands, g)

    def new_u(g):
        for cp in rs_pair(D_RS, part, d_lands, g, 1):
            cp.wait_send()
        total = rs_sum(D_RS, part, d_lands, g)
        total = pbuf[g, aligned(z, blk), :].astype(F32) + total
        pu[g, pl.ds(pl.multiple_of(k * half_rows + z * blk, blk), blk), :] = total.astype(BF16)
        ag_send(U_AG, u_blk, g, 1)

    def u_done(g):
        for cp in ag_wait(U_AG, u_blk, g, hops):
            cp.wait_recv()
        u_swap(g, k).start()

    head_tn = tile_of(q, 512)
    per_piece = q // head_tn

    def lane_stats(g, tile):
        unit = 16
        for i in range(rows // unit):
            r = slice(i * unit, (i + 1) * unit)
            parts = [zst[g, r, tile * head_tn + b * lanes:tile * head_tn + (b + 1) * lanes] for b in range(head_tn // lanes)]
            top = functools.reduce(jnp.maximum, parts)
            if tile == 0:
                total = jnp.zeros_like(top)
            else:
                old = mst[r, :]
                top = jnp.maximum(top, old)
                total = sst[r, :] * jnp.exp(old - top)
            for v in parts:
                total += jnp.exp(v - top)
            mst[r, :] = top
            sst[r, :] = total

    def head(g, j):
        if j == 0:
            u_swap(g, other).wait_recv()

            @pl.when(g == 0)
            def _():
                for i in range(n_dq):
                    for jj in range(n_vq):
                        head_copy(i, jj).wait()

            def put(r, v):
                obuf[r, :] = v

            norm_into(lambda r: pu[g, r, :], put, og, rows)

        for t in range(per_piece):
            tile = j * per_piece + t
            if tile > 0:
                lane_stats(g, tile - 1)
            weights = big[j * n_dq:(j + 1) * n_dq, :, t * head_tn:(t + 1) * head_tn].reshape(dim, head_tn)
            acc = jnp.dot(obuf[...], weights, preferred_element_type=F32)
            zst[g, :, tile * head_tn:(tile + 1) * head_tn] = acc

    def row_stats(g):
        lane_stats(g, n_vq * per_piece - 1)
        m = mst[...]
        top = jnp.max(m, axis=-1, keepdims=True)
        s = jnp.sum(sst[...] * jnp.exp(m - top), axis=-1, keepdims=True)
        mt = jnp.broadcast_to(top, mst.shape).T
        st = jnp.broadcast_to(s, sst.shape).T
        n = rows // lanes
        for i in range(n):
            c = slice(i * lanes, (i + 1) * lanes)
            stats[g, me, i:i + 1, :] = mt[0:1, c]
            stats[g, me, n + i:n + i + 1, :] = st[0:1, c]
        for d in range(1, n_tp):
            stat_send(g, d).start()

    def total_lse(g):
        for d in range(1, n_tp):
            stat_wait(g, d).wait_recv()
        n = rows // lanes
        ms = [stats[g, i, 0:n, :] for i in range(n_tp)]
        top = functools.reduce(jnp.maximum, ms)
        tot = functools.reduce(jnp.add, [stats[g, i, n:2 * n, :] * jnp.exp(ms[i] - top) for i in range(n_tp)])
        total = top + jnp.log(tot)
        for i in range(n):
            lse[g, i * lanes:(i + 1) * lanes, :] = columns_of(total[i:i + 1, :], lanes)

    bind = functools.partial
    stages = [[bind(picks, j=j) for j in range(n_dq)], [pick_sum]]
    stages += [[bind(rs_step, E_RS, land, e_lands, s=s)] for s in range(2, hops + 1)]
    stages += [[e_norm]]
    stages += [[bind(ag_step, E_AG, e_blk, s=s)] for s in range(2, hops + 1)]
    stages[-1].append(h_norm)
    stages += [[project]]
    stages += [[bind(ag_step, P_AG, p_blk, s=s)] for s in range(2, hops + 1)]
    stages += [[bind(ffn_up, first=True), bind(ffn_up, first=False), ffn_down]]
    stages += [[bind(rs_step, D_RS, part, d_lands, s=s)] for s in range(2, hops + 1)]
    stages += [[new_u]]
    stages += [[bind(ag_step, U_AG, u_blk, s=s)] for s in range(2, hops + 1)]
    stages += [[u_done]]
    stages += [[bind(head, j=j) for j in range(n_vq)] + [row_stats]]
    stages += [[total_lse]]
    last = len(stages) - 1
    order = []
    for i, pieces in enumerate(stages):
        for p in range(len(pieces)):
            place = (1.0 if i == last else -1.5 if (i, p) == (0, 0) else -i + p * 1.0, p > 0)
            order.append((place, i, p))
    order.sort()

    one_hot(0)
    for j in range(n_dq):
        for i in range(n_vq):
            emb_copy(i, j).wait()
        if j == n_dq - 1:
            for c in w_local:
                c.start()

            @pl.loop(0, groups)
            def _(g):
                hid_copy(g).start()

        pick_cols(0, j)
    pl.semaphore_wait(barrier, n_tp - 1)
    pick_swap(0).start()
    w_local[0].wait()
    w_send[0].start()

    @pl.loop(1, groups + last)
    def _(t):
        for _, i, p in order:
            g = t - i

            @pl.when((g >= 0) & (g < groups))
            def _():
                stages[i][p](g=g)

    for cp in w_send:
        cp.wait_send()

    @pl.loop(0, groups)
    def _(g):
        for s in range(1, hops + 1):
            for cp in rs_pair(E_RS, land, e_lands, g, s):
                cp.wait_send()
            if s > 1:
                for cp in rs_pair(D_RS, part, d_lands, g, s):
                    cp.wait_send()
            for c, b in ((E_AG, e_blk), (P_AG, p_blk), (U_AG, u_blk)):
                for cp in ag_pair(c, b, g, s):
                    cp.wait_send()
        u_swap(g, k).wait_send()
        for d in range(1, n_tp):
            stat_send(g, d).wait_send()


def finish_kernel(z, lse, pu, logp, u, sem):
    i = pl.program_id(0)
    n_rows, vocab = logp.shape
    unit, lanes = 16, lse.shape[1]
    u_copy = pltpu.make_async_copy(pu, u, sem)

    @pl.when(i == 0)
    def _():
        u_copy.start()

    @pl.loop(0, n_rows // unit)
    def _(c):
        r = aligned(i * (n_rows // unit) + c, unit)
        base = lse[r, :]
        for j in range(vocab // lanes):
            cols = slice(j * lanes, (j + 1) * lanes)
            logp[aligned(c, unit), cols] = z[r, cols] - base

    @pl.when(i == pl.num_programs(0) - 1)
    def _():
        u_copy.wait()


def finish_call(z, lse, pu):
    batch, vocab = z.shape
    vm = pl.BlockSpec(memory_space=pltpu.VMEM)
    step = GROUP_ROWS
    return pl.pallas_call(
        finish_kernel,
        grid=(batch // step,),
        out_shape=(jax.ShapeDtypeStruct((batch, vocab), F32), jax.ShapeDtypeStruct(pu.shape, BF16)),
        in_specs=[vm, vm, vm],
        out_specs=(pl.BlockSpec((step, vocab), lambda i: (i, 0)), pl.BlockSpec(memory_space=pltpu.HBM)),
        scratch_shapes=[pltpu.SemaphoreType.DMA],
        compiler_params=pltpu.CompilerParams(vmem_limit_bytes=16 << 20),
        name="finish",
    )(z, lse, pu)


def draft_call(n_tp, hidden, tokens, embedding, head_w, h_norm, e_norm, f_norm, o_norm, proj_w, w_gate, w_up, w_down):
    batch, dim = hidden.shape
    vocab = embedding.shape[0]
    pcols, fcols = proj_w.shape[1], w_gate.shape[1]
    groups = batch // GROUP_ROWS
    half_rows = GROUP_ROWS // CORES
    chips = n_tp // CORES
    hops = chips // 2
    blk = half_rows // chips
    q = dim // 2
    lanes = 128
    tok = tokens.reshape(batch // lanes, lanes)
    vm = pl.BlockSpec(memory_space=pltpu.VMEM)
    hbm = pl.BlockSpec(memory_space=pltpu.HBM)
    dma = pltpu.SemaphoreType.DMA
    n_big = (vocab // q) * (dim // q)
    flops = 2 * batch * (2 * dim * vocab + 2 * dim * pcols + 3 * dim * fcols)
    return pl.pallas_call(
        functools.partial(step_kernel, n_tp),
        out_shape=(
            pltpu.VMEM((groups, GROUP_ROWS, dim), BF16),
            pltpu.VMEM((groups, GROUP_ROWS, vocab), F32),
            pltpu.VMEM((groups, GROUP_ROWS, lanes), F32),
        ),
        in_specs=[vm] * 5 + [hbm] * 7,
        out_specs=(vm, vm, vm),
        scratch_shapes=[
            pltpu.VMEM((n_big, q, q), BF16),
            pltpu.VMEM((groups, half_rows, dim), BF16),
            pltpu.VMEM((groups, half_rows, dim), BF16),
            pltpu.VMEM((groups, half_rows, dim), BF16),
            pltpu.VMEM((groups, half_rows, dim), BF16),
            pltpu.VMEM((2 * dim, CORES * pcols), BF16),
            pltpu.VMEM((dim, CORES * fcols), BF16),
            pltpu.VMEM((dim, CORES * fcols), BF16),
            pltpu.VMEM((CORES * fcols, dim), BF16),
            pltpu.VMEM((groups, hops, blk, dim), BF16),
            pltpu.VMEM((groups, hops, blk, dim), BF16),
            pltpu.VMEM((groups, hops, blk, dim), F32),
            pltpu.VMEM((groups, hops, blk, dim), F32),
            pltpu.VMEM((GROUP_ROWS, vocab), BF16),
            pltpu.VMEM((GROUP_ROWS, lanes), F32),
            pltpu.VMEM((GROUP_ROWS, lanes), F32),
            pltpu.VMEM((GROUP_ROWS, lanes), F32),
            pltpu.VMEM((groups, n_tp, 8, lanes), F32),
            dma((5, 4, groups, hops)),
            dma((2, groups)),
            dma((2, groups)),
            dma((4,)),
            dma((4,)),
            dma((groups, n_tp)),
            dma((groups, n_tp)),
            dma((4 + groups,)),
            dma((n_big,)),
            dma((n_big,)),
        ],
        compiler_params=pltpu.CompilerParams(
            collective_id=0, has_side_effects=True, vmem_limit_bytes=KERNEL_VMEM),
        cost_estimate=pl.CostEstimate(flops=flops, bytes_accessed=70 << 20, transcendentals=0),
        name="draft_step",
    )(tok, h_norm[None], e_norm[None], f_norm[None], o_norm[None], hidden, embedding, head_w, proj_w, w_gate, w_up, w_down)


def solution(mesh):
    n_tp = mesh.shape["tp"]

    def draft_step(hidden, *rest):
        batch, dim = hidden.shape
        pu, z, lse = draft_call(n_tp, hidden, *rest)
        logp, new_u = finish_call(z.reshape(batch, -1), lse.reshape(batch, -1), pu.reshape(batch, dim))
        return new_u, logp

    specs_in = (P("dp", None), P("dp"), P("tp", None), P(None, "tp"), P(None), P(None), P(None), P(None), P(None, "tp"), P(None, "tp"), P(None, "tp"), P("tp", None))
    specs_out = (P("dp", None), P("dp", "tp"))
    return jax.shard_map(draft_step, mesh=mesh, in_specs=specs_in, out_specs=specs_out, check_vma=False)
```

```python
import functools

import jax
import jax.numpy as jnp
from jax import lax
from jax.experimental import pallas as pl
from jax.experimental.pallas import tpu as pltpu
from jax.sharding import PartitionSpec as P

NORM_EPS = 1e-6
BF16 = jnp.bfloat16
F32 = jnp.float32
GROUP_ROWS = 256
KERNEL_VMEM = 47 << 20
CORES = 2
SEND_R, SEND_L, FROM_L, FROM_R = range(4)
E_RS, E_AG, P_AG, D_RS, U_AG = range(5)


def norm_rows(values, gain):
    wide = values.astype(F32)
    inv = lax.rsqrt(jnp.mean(wide * wide, axis=-1, keepdims=True) + NORM_EPS)
    return wide * inv * gain


def norm_into(load, store, gain, n_rows, unit=16, width=4):
    width = min(width, n_rows // unit)

    @pl.loop(0, n_rows // (unit * width))
    def _(i):
        rows = [pl.ds(pl.multiple_of((i * width + u) * unit, unit), unit) for u in range(width)]
        scales = []
        for r in rows:
            wide = load(r).astype(F32)
            scales.append(lax.rsqrt(jnp.mean(wide * wide, axis=-1, keepdims=True) + NORM_EPS))
        for r, inv in zip(rows, scales):
            store(r, (load(r).astype(F32) * inv * gain[...]).astype(BF16))


def columns_of(row, lanes):
    return jnp.broadcast_to(row, (lanes, lanes)).T


def aligned(index, size):
    return pl.ds(pl.multiple_of(index * size, size), size)


def tile_of(width, most):
    return min(width, most)


def step_kernel(
    n_tp, tok, hg, eg, fg, og, hid_h, emb_h, head_h, pw_h, wg_h, wu_h, wd_h,
    pu, zst, lse,
    big, hid, land, ebuf, pbuf, pw, wg, wu, wd, erl, err, drl, drr,
    onehot, obuf, ids_ref, mst, sst, stats,
    ring, xsend, xrecv, wsend, wrecv, ssend, srecv, lsem, bsem, hsem,
):
    groups, half_rows, dim = hid.shape
    chips = n_tp // CORES
    hops = chips // 2
    rows = CORES * half_rows
    blk = half_rows // chips
    hcol = dim // 2
    hrow = half_rows // 2
    pcols = pw.shape[1] // CORES
    fcols = wg.shape[1] // CORES
    vocab = zst.shape[2]
    lanes = stats.shape[3]
    part = zst.at[:, pl.ds(0, half_rows), pl.ds(0, dim)]
    width = wg.shape[1]
    nbuf = onehot.at[pl.ds(0, half_rows), pl.ds(0, dim)]
    abuf = onehot.at[pl.ds(half_rows, half_rows), pl.ds(0, width)]
    q = big.shape[1]
    n_vq, n_dq = vocab // q, dim // q

    me = lax.axis_index("tp")
    z, k = me // CORES, lax.rem(me, CORES)
    other = 1 - k
    sib = z * CORES + other
    right = lax.rem(me + CORES, n_tp)
    left = lax.rem(me + n_tp - CORES, n_tp)

    def chip(offset):
        return lax.rem(z + offset + chips, chips)

    def remote(src, dst, ssem, rsem, dev):
        return pltpu.make_async_remote_copy(
            src_ref=src, dst_ref=dst, send_sem=ssem, recv_sem=rsem,
            device_id={"tp": dev}, device_id_type=pl.DeviceIdType.MESH,
        )

    def emb_copy(i, j, h):
        w = q // 2
        return pltpu.make_async_copy(
            emb_h.at[pl.ds(i * q, q), pl.ds(j * q + h * w, w)], big.at[j * n_vq + i, :, pl.ds(h * w, w)], bsem.at[(j * n_vq + i) * 2 + h])

    def head_copy(i, j):
        return pltpu.make_async_copy(
            head_h.at[pl.ds(i * q, q), pl.ds(j * q, q)], big.at[j * n_dq + i], hsem.at[j * n_dq + i])

    def hid_copy(g):
        return pltpu.make_async_copy(
            hid_h.at[pl.ds(pl.multiple_of(g * rows + k * half_rows, half_rows), half_rows)], hid.at[g], lsem.at[4 + g])

    own_pw = pw.at[:, aligned(k, pcols)]
    own_wg = wg.at[:, aligned(k, fcols)]
    own_wu = wu.at[:, aligned(k, fcols)]
    own_wd = wd.at[aligned(k, fcols), :]
    oth_pw = pw.at[:, aligned(other, pcols)]
    oth_wg = wg.at[:, aligned(other, fcols)]
    oth_wu = wu.at[:, aligned(other, fcols)]
    oth_wd = wd.at[aligned(other, fcols), :]
    w_local = [pltpu.make_async_copy(s, d, lsem.at[i]) for i, (s, d) in enumerate(
        [(pw_h, own_pw), (wg_h, own_wg), (wu_h, own_wu), (wd_h, own_wd)])]
    w_send = [remote(r, r, wsend.at[i], wrecv.at[i], sib) for i, r in enumerate([own_pw, own_wg, own_wu, own_wd])]
    w_recv = [remote(r, r, wsend.at[i], wrecv.at[i], sib) for i, r in enumerate([oth_pw, oth_wg, oth_wu, oth_wd])]

    barrier = pltpu.get_barrier_semaphore()
    for d in range(1, n_tp):
        pl.semaphore_signal(barrier, inc=1, device_id={"tp": lax.rem(me + d, n_tp)}, device_id_type=pl.DeviceIdType.MESH)
    for j in range(n_dq):
        for h in range(2):
            for i in range(n_vq):
                emb_copy(i, j, h).start()

    def e_blk(g, o, h):
        cols = pl.ds(0, dim) if h is None else pl.ds(h * hcol, hcol)
        return ebuf.at[g, aligned(o, blk), cols]

    def p_blk(g, o, h):
        r = pl.ds(0, half_rows) if h is None else pl.ds(h * hrow, hrow)
        return pbuf.at[g, r, aligned(o, CORES * pcols)]

    def u_blk(g, o, h):
        cols = pl.ds(0, dim) if h is None else pl.ds(h * hcol, hcol)
        return pu.at[g, pl.ds(pl.multiple_of(k * half_rows + o * blk, blk), blk), cols]

    def ag_pair(c, block, g, s):
        last = s == hops
        r = block(g, chip(-(s - 1)), 0 if last else None)
        l = block(g, chip(s - 1), 1 if last else None)
        return (remote(r, r, ring.at[c, SEND_R, g, s - 1], ring.at[c, FROM_L, g, s - 1], right),
                remote(l, l, ring.at[c, SEND_L, g, s - 1], ring.at[c, FROM_R, g, s - 1], left))

    def ag_wait(c, block, g, s):
        last = s == hops
        r = block(g, chip(-s), 0 if last else None)
        l = block(g, chip(s), 1 if last else None)
        return (remote(r, r, ring.at[c, SEND_R, g, s - 1], ring.at[c, FROM_L, g, s - 1], right),
                remote(l, l, ring.at[c, SEND_L, g, s - 1], ring.at[c, FROM_R, g, s - 1], left))

    def ag_send(c, block, g, s):
        for cp in ag_pair(c, block, g, s):
            cp.start()

    def ag_step(c, block, g, s):
        got, send = ag_wait(c, block, g, s - 1), ag_pair(c, block, g, s)
        for a, b in zip(got, send):
            a.wait_recv()
            b.start()

    def rs_part(ref, h):
        return ref if h is None else ref.at[:, pl.ds(h * hcol, hcol)]

    def rs_pair(c, own, lands, g, s):
        out = []
        for kind, frm, side, dev, h1, sign in ((SEND_R, FROM_L, 0, right, 0, 1), (SEND_L, FROM_R, 1, left, 1, -1)):
            h = h1 if s == 1 else None
            dst = rs_part(lands[side].at[g, s - 1], h)
            src = rs_part(own.at[g, aligned(chip(sign * hops), blk)], h) if s == 1 else lands[side].at[g, s - 2]
            out.append(remote(src, dst, ring.at[c, kind, g, s - 1], ring.at[c, frm, g, s - 1], dev))
        return out

    def rs_wait(c, own, lands, g, s):
        return rs_pair(c, own, lands, g, s)

    def rs_first(c, own, lands, g):
        for cp in rs_pair(c, own, lands, g, 1):
            cp.start()

    def rs_step(c, own, lands, g, s):
        got, send = rs_wait(c, own, lands, g, s - 1), rs_pair(c, own, lands, g, s)
        for side, sign in ((0, 1), (1, -1)):
            got[side].wait_recv()
            o = aligned(chip(sign * (hops + 1 - s)), blk)
            slot = lands[side].at[g, s - 2]
            if s == 2:
                for h in range(2):
                    c_ = slice(h * hcol, (h + 1) * hcol)
                    mine = own[g, o, c_]
                    slot[:, c_] = slot[:, c_] + mine if h == side else mine
            else:
                slot[...] = slot[...] + own[g, o, :]
            send[side].start()

    def rs_sum(c, own, lands, g):
        for cp in rs_wait(c, own, lands, g, hops):
            cp.wait_recv()
        mine = own[g, aligned(z, blk), :]
        return lands[0][g, hops - 1].astype(F32) + mine.astype(F32) + lands[1][g, hops - 1].astype(F32)

    e_lands, d_lands = (erl, err), (drl, drr)

    def pick_swap(g):
        return remote(pu.at[g, aligned(other, half_rows)], land.at[g], xsend.at[0, g], xrecv.at[0, g], sib)

    def u_swap(g, c):
        r = pu.at[g, aligned(c, half_rows)]
        return remote(r, r, xsend.at[1, g], xrecv.at[1, g], sib)

    def stat_send(g, d):
        return remote(stats.at[g, me], stats.at[g, me], ssend.at[g, d], srecv.at[g, d], lax.rem(me + d, n_tp))

    def stat_wait(g, d):
        src = lax.rem(me + n_tp - d, n_tp)
        return remote(stats.at[g, src], stats.at[g, src], ssend.at[g, d], srecv.at[g, d], lax.rem(me + d, n_tp))

    def one_hot(g):
        per = rows // lanes
        for i in range(per):
            row = (tok[pl.ds(g * per + i, 1), :] - me * vocab).astype(F32)
            ids_ref[i * lanes:(i + 1) * lanes, :] = columns_of(row, lanes)
        lane = lax.broadcasted_iota(jnp.int32, (rows, lanes), 1)

        @pl.loop(0, vocab // lanes, unroll=4)
        def _(j):
            here = (lane + j * lanes).astype(F32)
            onehot[:, aligned(j, lanes)] = jnp.where(ids_ref[...] == here, 1.0, 0.0).astype(BF16)

    def pick_cols(g, j, tn, t=0):
        table = big[j * n_vq:(j + 1) * n_vq, :, t * tn:(t + 1) * tn].reshape(vocab, tn)
        acc = jnp.dot(onehot[...], table, preferred_element_type=F32)
        pu[g, :, j * q + t * tn:j * q + (t + 1) * tn] = acc.astype(BF16)

    def picks(g, j):
        @pl.when(g > 0)
        def _():
            if j == 0:
                one_hot(g)
            pick_cols(g, j, q)
            if j == n_dq - 1:
                pick_swap(g).start()

        if j == n_dq - 1:
            @pl.when(g == groups - 1)
            def _():
                for i in range(n_dq):
                    for jj in range(n_vq):
                        head_copy(i, jj).start()

    def pick_sum(g):
        pick_swap(g).wait_recv()

        for i in range(chips):
            r = pl.ds(i * blk, blk)
            land[g, r, :] = land[g, r, :] + pu[g, pl.ds(pl.multiple_of(k * half_rows + i * blk, blk), blk), :]

        rs_first(E_RS, land, e_lands, g)

    def e_norm(g):
        pick_swap(g).wait_send()
        ebuf[g, aligned(z, blk), :] = norm_rows(rs_sum(E_RS, land, e_lands, g), eg[...]).astype(BF16)
        ag_send(E_AG, e_blk, g, 1)

    def h_norm(g):
        hid_copy(g).wait()

        def put(r, v):
            hid[g, r, :] = v

        norm_into(lambda r: hid[g, r, :], put, hg, half_rows)

        @pl.when(g == 0)
        def _():
            for i in range(1, 4):
                w_local[i].wait()
                w_send[i].start()

    def project(g):
        for cp in ag_wait(E_AG, e_blk, g, hops):
            cp.wait_recv()

        @pl.when(g == 0)
        def _():
            w_recv[0].wait_recv()

        out = jnp.dot(hid[g], pw[:dim, :], preferred_element_type=F32)
        out += jnp.dot(ebuf[g], pw[dim:, :], preferred_element_type=F32)
        pbuf[g, :, aligned(z, CORES * pcols)] = out.astype(BF16)
        ag_send(P_AG, p_blk, g, 1)

    def ffn_up(g, first):
        if first:
            for cp in ag_wait(P_AG, p_blk, g, hops):
                cp.wait_recv()

            @pl.when(g == 0)
            def _():
                for i in range(1, 4):
                    w_recv[i].wait_recv()

            def put(r, v):
                nbuf[r, :] = v

            norm_into(lambda r: pbuf[g, r, :], put, fg, half_rows)

        tn = tile_of(width, 256)
        n = width // tn
        lo, hi = (0, n // 2) if first else (n // 2, n)

        @pl.loop(lo, hi)
        def _(t):
            c = aligned(t, tn)
            gate = jnp.dot(nbuf[...], wg[:, c], preferred_element_type=F32)
            up = jnp.dot(nbuf[...], wu[:, c], preferred_element_type=F32)
            abuf[:, c] = (jax.nn.silu(gate) * up).astype(BF16)

    def ffn_down(g):
        tm = tile_of(dim, 512)

        @pl.loop(0, dim // tm)
        def _(t):
            c = aligned(t, tm)
            part[g, :, c] = jnp.dot(abuf[...], wd[:, c], preferred_element_type=F32)

        rs_first(D_RS, part, d_lands, g)

    def new_u(g):
        for cp in rs_pair(D_RS, part, d_lands, g, 1):
            cp.wait_send()
        total = rs_sum(D_RS, part, d_lands, g)
        total = pbuf[g, aligned(z, blk), :].astype(F32) + total
        pu[g, pl.ds(pl.multiple_of(k * half_rows + z * blk, blk), blk), :] = total.astype(BF16)
        ag_send(U_AG, u_blk, g, 1)

    def o_half(g, c):
        slot = lax.rem(g, 2)

        def at(r):
            return pl.ds(pl.multiple_of(c * half_rows + r.start, 16), r.size)

        def put(r, v):
            obuf[slot, at(r), :] = v

        norm_into(lambda r: pu[g, at(r), :], put, og, half_rows)

    def u_done(g):
        for cp in ag_wait(U_AG, u_blk, g, hops):
            cp.wait_recv()
        u_swap(g, k).start()
        o_half(g, k)

    head_tn = tile_of(q, 512)
    per_piece = q // head_tn

    def lane_stats(g, tile):
        unit = 16
        for i in range(rows // unit):
            r = slice(i * unit, (i + 1) * unit)
            parts = [zst[g, r, tile * head_tn + b * lanes:tile * head_tn + (b + 1) * lanes] for b in range(head_tn // lanes)]
            top = functools.reduce(jnp.maximum, parts)
            if tile == 0:
                total = jnp.zeros_like(top)
            else:
                old = mst[r, :]
                top = jnp.maximum(top, old)
                total = sst[r, :] * jnp.exp(old - top)
            for v in parts:
                total += jnp.exp(v - top)
            mst[r, :] = top
            sst[r, :] = total

    def head(g, j):
        if j == 0:
            u_swap(g, other).wait_recv()

            @pl.when(g == 0)
            def _():
                for i in range(n_dq):
                    for jj in range(n_vq):
                        head_copy(i, jj).wait()

            o_half(g, other)

        for t in range(per_piece):
            tile = j * per_piece + t
            if tile > 0:
                lane_stats(g, tile - 1)
            weights = big[j * n_dq:(j + 1) * n_dq, :, t * head_tn:(t + 1) * head_tn].reshape(dim, head_tn)
            acc = jnp.dot(obuf[lax.rem(g, 2)], weights, preferred_element_type=F32)
            zst[g, :, tile * head_tn:(tile + 1) * head_tn] = acc

    def row_stats(g):
        lane_stats(g, n_vq * per_piece - 1)
        m = mst[...]
        top = jnp.max(m, axis=-1, keepdims=True)
        s = jnp.sum(sst[...] * jnp.exp(m - top), axis=-1, keepdims=True)
        mt = jnp.broadcast_to(top, mst.shape).T
        st = jnp.broadcast_to(s, sst.shape).T
        n = rows // lanes
        for i in range(n):
            c = slice(i * lanes, (i + 1) * lanes)
            stats[g, me, i:i + 1, :] = mt[0:1, c]
            stats[g, me, n + i:n + i + 1, :] = st[0:1, c]
        for d in range(1, n_tp):
            stat_send(g, d).start()

    def total_lse(g):
        for d in range(1, n_tp):
            stat_wait(g, d).wait_recv()
        n = rows // lanes
        ms = [stats[g, i, 0:n, :] for i in range(n_tp)]
        top = functools.reduce(jnp.maximum, ms)
        tot = functools.reduce(jnp.add, [stats[g, i, n:2 * n, :] * jnp.exp(ms[i] - top) for i in range(n_tp)])
        total = top + jnp.log(tot)
        for i in range(n):
            lse[g, i * lanes:(i + 1) * lanes, :] = columns_of(total[i:i + 1, :], lanes)

    bind = functools.partial
    stages = [[bind(picks, j=j) for j in range(n_dq)], [pick_sum]]
    stages += [[bind(rs_step, E_RS, land, e_lands, s=s)] for s in range(2, hops + 1)]
    stages += [[e_norm]]
    stages += [[bind(ag_step, E_AG, e_blk, s=s)] for s in range(2, hops + 1)]
    stages[-1].append(h_norm)
    stages += [[project]]
    stages += [[bind(ag_step, P_AG, p_blk, s=s)] for s in range(2, hops + 1)]
    stages += [[bind(ffn_up, first=True), bind(ffn_up, first=False), ffn_down]]
    stages += [[bind(rs_step, D_RS, part, d_lands, s=s)] for s in range(2, hops + 1)]
    stages += [[new_u]]
    stages += [[bind(ag_step, U_AG, u_blk, s=s)] for s in range(2, hops + 1)]
    stages += [[u_done]]
    stages += [[bind(head, j=j) for j in range(n_vq)] + [row_stats]]
    stages += [[total_lse]]
    last = len(stages) - 1
    order = []
    for i, pieces in enumerate(stages):
        for p in range(len(pieces)):
            place = (1.0 if i == last else -3.5 if (i, p) == (0, 0) else -i + p * 1.0, p > 0)
            order.append((place, i, p))
    order.sort()

    one_hot(0)
    for j in range(n_dq):
        for h in range(2):
            for i in range(n_vq):
                emb_copy(i, j, h).wait()
            if (j, h) == (n_dq - 1, 1):
                for c in w_local:
                    c.start()

                @pl.loop(0, groups)
                def _(g):
                    hid_copy(g).start()

            pick_cols(0, j, q // 2, h)
    pl.semaphore_wait(barrier, n_tp - 1)
    pick_swap(0).start()
    w_local[0].wait()
    w_send[0].start()

    @pl.loop(1, groups + last)
    def _(t):
        for _, i, p in order:
            g = t - i

            @pl.when((g >= 0) & (g < groups))
            def _():
                stages[i][p](g=g)

    for cp in w_send:
        cp.wait_send()

    @pl.loop(0, groups)
    def _(g):
        for s in range(1, hops + 1):
            for cp in rs_pair(E_RS, land, e_lands, g, s):
                cp.wait_send()
            if s > 1:
                for cp in rs_pair(D_RS, part, d_lands, g, s):
                    cp.wait_send()
            for c, b in ((E_AG, e_blk), (P_AG, p_blk), (U_AG, u_blk)):
                for cp in ag_pair(c, b, g, s):
                    cp.wait_send()
        u_swap(g, k).wait_send()
        for d in range(1, n_tp):
            stat_send(g, d).wait_send()


def finish_kernel(z, lse, pu, logp, u, sem):
    i = pl.program_id(0)
    n_rows, vocab = logp.shape
    unit, lanes = 16, lse.shape[1]
    u_copy = pltpu.make_async_copy(pu, u, sem)

    @pl.when(i == 0)
    def _():
        u_copy.start()

    @pl.loop(0, n_rows // unit)
    def _(c):
        r = aligned(i * (n_rows // unit) + c, unit)
        base = lse[r, :]
        for j in range(vocab // lanes):
            cols = slice(j * lanes, (j + 1) * lanes)
            logp[aligned(c, unit), cols] = z[r, cols] - base

    @pl.when(i == pl.num_programs(0) - 1)
    def _():
        u_copy.wait()


def finish_call(z, lse, pu):
    batch, vocab = z.shape
    vm = pl.BlockSpec(memory_space=pltpu.VMEM)
    step = GROUP_ROWS
    return pl.pallas_call(
        finish_kernel,
        grid=(batch // step,),
        out_shape=(jax.ShapeDtypeStruct((batch, vocab), F32), jax.ShapeDtypeStruct(pu.shape, BF16)),
        in_specs=[vm, vm, vm],
        out_specs=(pl.BlockSpec((step, vocab), lambda i: (i, 0)), pl.BlockSpec(memory_space=pltpu.HBM)),
        scratch_shapes=[pltpu.SemaphoreType.DMA],
        compiler_params=pltpu.CompilerParams(vmem_limit_bytes=16 << 20),
        name="finish",
    )(z, lse, pu)


def draft_call(n_tp, hidden, tokens, embedding, head_w, h_norm, e_norm, f_norm, o_norm, proj_w, w_gate, w_up, w_down):
    batch, dim = hidden.shape
    vocab = embedding.shape[0]
    pcols, fcols = proj_w.shape[1], w_gate.shape[1]
    groups = batch // GROUP_ROWS
    half_rows = GROUP_ROWS // CORES
    chips = n_tp // CORES
    hops = chips // 2
    blk = half_rows // chips
    q = dim // 2
    lanes = 128
    tok = tokens.reshape(batch // lanes, lanes)
    vm = pl.BlockSpec(memory_space=pltpu.VMEM)
    hbm = pl.BlockSpec(memory_space=pltpu.HBM)
    dma = pltpu.SemaphoreType.DMA
    n_big = (vocab // q) * (dim // q)
    flops = 2 * batch * (2 * dim * vocab + 2 * dim * pcols + 3 * dim * fcols)
    return pl.pallas_call(
        functools.partial(step_kernel, n_tp),
        out_shape=(
            pltpu.VMEM((groups, GROUP_ROWS, dim), BF16),
            pltpu.VMEM((groups, GROUP_ROWS, vocab), F32),
            pltpu.VMEM((groups, GROUP_ROWS, lanes), F32),
        ),
        in_specs=[vm] * 5 + [hbm] * 7,
        out_specs=(vm, vm, vm),
        scratch_shapes=[
            pltpu.VMEM((n_big, q, q), BF16),
            pltpu.VMEM((groups, half_rows, dim), BF16),
            pltpu.VMEM((groups, half_rows, dim), BF16),
            pltpu.VMEM((groups, half_rows, dim), BF16),
            pltpu.VMEM((groups, half_rows, dim), BF16),
            pltpu.VMEM((2 * dim, CORES * pcols), BF16),
            pltpu.VMEM((dim, CORES * fcols), BF16),
            pltpu.VMEM((dim, CORES * fcols), BF16),
            pltpu.VMEM((CORES * fcols, dim), BF16),
            pltpu.VMEM((groups, hops, blk, dim), BF16),
            pltpu.VMEM((groups, hops, blk, dim), BF16),
            pltpu.VMEM((groups, hops, blk, dim), F32),
            pltpu.VMEM((groups, hops, blk, dim), F32),
            pltpu.VMEM((GROUP_ROWS, vocab), BF16),
            pltpu.VMEM((2, GROUP_ROWS, dim), BF16),
            pltpu.VMEM((GROUP_ROWS, lanes), F32),
            pltpu.VMEM((GROUP_ROWS, lanes), F32),
            pltpu.VMEM((GROUP_ROWS, lanes), F32),
            pltpu.VMEM((groups, n_tp, 8, lanes), F32),
            dma((5, 4, groups, hops)),
            dma((2, groups)),
            dma((2, groups)),
            dma((4,)),
            dma((4,)),
            dma((groups, n_tp)),
            dma((groups, n_tp)),
            dma((4 + groups,)),
            dma((2 * n_big,)),
            dma((n_big,)),
        ],
        compiler_params=pltpu.CompilerParams(
            collective_id=0, has_side_effects=True, vmem_limit_bytes=KERNEL_VMEM),
        cost_estimate=pl.CostEstimate(flops=flops, bytes_accessed=70 << 20, transcendentals=0),
        name="draft_step",
    )(tok, h_norm[None], e_norm[None], f_norm[None], o_norm[None], hidden, embedding, head_w, proj_w, w_gate, w_up, w_down)


def solution(mesh):
    n_tp = mesh.shape["tp"]

    def draft_step(hidden, *rest):
        batch, dim = hidden.shape
        pu, z, lse = draft_call(n_tp, hidden, *rest)
        logp, new_u = finish_call(z.reshape(batch, -1), lse.reshape(batch, -1), pu.reshape(batch, dim))
        return new_u, logp

    specs_in = (P("dp", None), P("dp"), P("tp", None), P(None, "tp"), P(None), P(None), P(None), P(None), P(None, "tp"), P(None, "tp"), P(None, "tp"), P("tp", None))
    specs_out = (P("dp", None), P("dp", "tp"))
    return jax.shard_map(draft_step, mesh=mesh, in_specs=specs_in, out_specs=specs_out, check_vma=False)
```
